8 devices in a mesh: dp: 1 (over z), tp: 2 (over y), sp: 4 (over x, core).
Axes of the slice: x: 2, y: 2, z: 1, core: 2. Of those that a mesh axis runs over, the one named last changes fastest.
Arguments:
- hidden: bfloat16 [4, 128, 4096], P(None, 'dp')
- start_pos: int32 [128], P('dp')
- k_cache: bfloat16 [128, 1024, 8, 128], P('dp', 'sp', 'tp')
- v_cache: bfloat16 [128, 1024, 8, 128], P('dp', 'sp', 'tp')
- w_q: bfloat16 [4096, 4096], P(None, 'tp')
- w_k: bfloat16 [4096, 1024], P(None, 'tp')
- w_v: bfloat16 [4096, 1024], P(None, 'tp')
- w_o: bfloat16 [4096, 4096], P('tp')
- w_gate: bfloat16 [4096, 12288], P(None, 'tp')
- w_up: bfloat16 [4096, 12288], P(None, 'tp')
- w_down: bfloat16 [12288, 4096], P('tp')
- attn_norm: bfloat16 [4096], replicated
- mlp_norm: bfloat16 [4096], replicated
- q_gain: bfloat16 [128], replicated
- k_gain: bfloat16 [128], replicated
Outputs:
- output 1: bfloat16 [4, 128, 4096], P(None, 'dp')
- output 2: bfloat16 [128, 1024, 8, 128], P('dp', 'sp', 'tp')
- output 3: bfloat16 [128, 1024, 8, 128], P('dp', 'sp', 'tp')
All inputs are finite; a program needn't handle non-finite values.
Results may differ from the reference program's by a relative error of at most 0.00856035.
Values sent between devices are 32-bit elements.
A program may use at most 1.5 GiB of HBM per device.

```python
import math
import jax
import jax.numpy as jnp
from jax import lax

D_MODEL = 4096
HEADS = 32
KV_HEADS = 8
FFN_DIM = 12288
HEAD_DIM = 128
STEPS = 4
BATCH = 128
SEQ_DEV = 256
SEQ_LEN = 1024
ROPE_BASE = 1000000.0
NORM_EPS = 1e-06


def rms_scale(values, gain_vec):
    wide_vals = values.astype(jnp.float32)
    inv_rms = lax.rsqrt(jnp.mean(wide_vals * wide_vals, axis=-1, keepdims=True) + NORM_EPS)
    return wide_vals * inv_rms * gain_vec.astype(jnp.float32)


def apply_rope(vector, tok_pos):
    head_dim = vector.shape[-1]
    half_dim = head_dim // 2
    freqs = ROPE_BASE ** (-(jnp.arange(half_dim, dtype=jnp.float32) * (2.0 / head_dim)))
    angles = tok_pos.astype(jnp.float32)[:, None] * freqs[None, :]
    cos_tab = jnp.cos(angles)[:, None, :]
    sin_tab = jnp.sin(angles)[:, None, :]
    lower_half = vector[..., :half_dim]
    upper_half = vector[..., half_dim:]
    return jnp.concatenate([lower_half * cos_tab - upper_half * sin_tab, upper_half * cos_tab + lower_half * sin_tab], axis=-1)


def setup_inputs(seed: int = 0, part: int = 0) -> dict:
    w_keys = jax.random.split(jax.random.key(seed), 11)
    part_keys = jax.random.split(jax.random.fold_in(jax.random.key(seed + 1), part), 5)
    q_width = HEADS * HEAD_DIM
    kv_width = KV_HEADS * HEAD_DIM
    q_scale = math.sqrt(math.log(SEQ_LEN / 16.0))
    k_scale = math.sqrt(2.0 * math.log(SEQ_LEN)) / 1.5

    def normal_draw(key_in, shape, scale):
        return (jax.random.normal(key_in, shape, jnp.float32) * scale).astype(jnp.bfloat16)

    def gain_draw(key_in, shape, scale):
        return (scale * (1.0 + 0.2 * jax.random.normal(key_in, shape, jnp.float32))).astype(jnp.bfloat16)

    drawn_pos = jax.random.randint(part_keys[1], (BATCH,), SEQ_DEV, SEQ_LEN - STEPS + 1, dtype=jnp.int32)
    order = jax.random.permutation(part_keys[2], BATCH)
    start_pos = drawn_pos.at[order[0]].set(SEQ_LEN - STEPS).at[order[1]].set(SEQ_DEV)
    filled = (jnp.arange(SEQ_LEN)[None, :] < start_pos[:, None])[:, :, None, None]
    cache_shape = (BATCH, SEQ_LEN, KV_HEADS, HEAD_DIM)
    k_cache = jnp.where(filled, jax.random.normal(part_keys[3], cache_shape, jnp.float32), 0.0).astype(jnp.bfloat16)
    v_cache = jnp.where(filled, jax.random.normal(part_keys[4], cache_shape, jnp.float32), 0.0).astype(jnp.bfloat16)
    return {
        'hidden': normal_draw(part_keys[0], (STEPS, BATCH, D_MODEL), 1.0),
        'start_pos': start_pos,
        'k_cache': k_cache,
        'v_cache': v_cache,
        'w_q': normal_draw(w_keys[0], (D_MODEL, q_width), D_MODEL ** -0.5),
        'w_k': normal_draw(w_keys[1], (D_MODEL, kv_width), D_MODEL ** -0.5),
        'w_v': normal_draw(w_keys[2], (D_MODEL, kv_width), D_MODEL ** -0.5),
        'w_o': normal_draw(w_keys[3], (q_width, D_MODEL), 2.0 * q_width ** -0.5),
        'w_gate': normal_draw(w_keys[4], (D_MODEL, FFN_DIM), D_MODEL ** -0.5),
        'w_up': normal_draw(w_keys[5], (D_MODEL, FFN_DIM), D_MODEL ** -0.5),
        'w_down': normal_draw(w_keys[6], (FFN_DIM, D_MODEL), FFN_DIM ** -0.5),
        'attn_norm': gain_draw(w_keys[7], (D_MODEL,), 1.0),
        'mlp_norm': gain_draw(w_keys[8], (D_MODEL,), 1.0),
        'q_gain': gain_draw(w_keys[9], (HEAD_DIM,), q_scale),
        'k_gain': gain_draw(w_keys[10], (HEAD_DIM,), k_scale),
    }


def reference(hidden, start_pos, k_cache, v_cache, w_q, w_k, w_v, w_o, w_gate, w_up, w_down, attn_norm, mlp_norm, q_gain, k_gain):
    groups = HEADS // KV_HEADS
    score_scale = HEAD_DIM ** -0.5
    seq_pos = jnp.arange(SEQ_LEN)

    def attend_one(request):
        q_one, k_one, v_one, pos_one = request
        scores = jnp.einsum('kgh,lkh->kgl', q_one.astype(jnp.float32), k_one.astype(jnp.float32)) * score_scale
        scores = jnp.where(seq_pos <= pos_one, scores, -jnp.inf)
        probs = jax.nn.softmax(scores, axis=-1)
        return jnp.einsum('kgl,lkh->kgh', probs, v_one.astype(jnp.float32))

    def decode_step(caches, step_in):
        k_all, v_all = caches
        x_tok, step_idx = step_in
        tok_pos = start_pos + step_idx
        normed = rms_scale(x_tok, attn_norm).astype(jnp.bfloat16)
        q_raw = jnp.dot(normed, w_q, preferred_element_type=jnp.float32).reshape(BATCH, HEADS, HEAD_DIM)
        k_raw = jnp.dot(normed, w_k, preferred_element_type=jnp.float32).reshape(BATCH, KV_HEADS, HEAD_DIM)
        v_new = jnp.dot(normed, w_v, preferred_element_type=jnp.float32).astype(jnp.bfloat16).reshape(BATCH, KV_HEADS, HEAD_DIM)
        q_rot = apply_rope(rms_scale(q_raw, q_gain), tok_pos).astype(jnp.bfloat16).reshape(BATCH, KV_HEADS, groups, HEAD_DIM)
        k_new = apply_rope(rms_scale(k_raw, k_gain), tok_pos).astype(jnp.bfloat16)
        hit = (seq_pos[None, :] == tok_pos[:, None])[:, :, None, None]
        k_all = jnp.where(hit, k_new[:, None], k_all)
        v_all = jnp.where(hit, v_new[:, None], v_all)
        attn_vals = lax.map(attend_one, (q_rot, k_all, v_all, tok_pos))
        attn_in = attn_vals.reshape(BATCH, HEADS * HEAD_DIM).astype(jnp.bfloat16)
        attn_out = jnp.dot(attn_in, w_o, preferred_element_type=jnp.float32)
        residual = (x_tok.astype(jnp.float32) + attn_out).astype(jnp.bfloat16)
        mlp_in = rms_scale(residual, mlp_norm).astype(jnp.bfloat16)
        gate_act = jnp.dot(mlp_in, w_gate, preferred_element_type=jnp.float32)
        up_proj = jnp.dot(mlp_in, w_up, preferred_element_type=jnp.float32)
        mlp_act = (jax.nn.silu(gate_act) * up_proj).astype(jnp.bfloat16)
        down_out = jnp.dot(mlp_act, w_down, preferred_element_type=jnp.float32)
        out_tok = (residual.astype(jnp.float32) + down_out).astype(jnp.bfloat16)
        return (k_all, v_all), out_tok

    final_caches, outputs = lax.scan(decode_step, (k_cache, v_cache), (hidden, jnp.arange(STEPS)))
    return outputs, final_caches[0], final_caches[1]
```

```python
import functools
import math

import jax
import jax.numpy as jnp
from jax import lax
from jax.experimental import pallas as pl
from jax.experimental.pallas import tpu as pltpu
from jax.sharding import PartitionSpec as P

ROPE_BASE = 1000000.0
NORM_EPS = 1e-06
MASKED = -3e38
FLOOR = -1e38


def rms_scale(values, gain_vec):
    wide_vals = values.astype(jnp.float32)
    inv_rms = lax.rsqrt(jnp.mean(wide_vals * wide_vals, axis=-1, keepdims=True) + NORM_EPS)
    return wide_vals * inv_rms * gain_vec.astype(jnp.float32)


def apply_rope(vector, tok_pos):
    head_dim = vector.shape[-1]
    half_dim = head_dim // 2
    freqs = ROPE_BASE ** (-(jnp.arange(half_dim, dtype=jnp.float32) * (2.0 / head_dim)))
    angles = tok_pos.astype(jnp.float32)[..., None] * freqs
    cos_tab = jnp.cos(angles)[..., None, :]
    sin_tab = jnp.sin(angles)[..., None, :]
    lower_half = vector[..., :half_dim]
    upper_half = vector[..., half_dim:]
    return jnp.concatenate([lower_half * cos_tab - upper_half * sin_tab, upper_half * cos_tab + lower_half * sin_tab], axis=-1)


def attn_kernel(dims, order_ref, rel_ref, q_ref, kn_ref, vn_ref, k_ref, v_ref, ko_ref, vo_ref, o_ref, ml_ref):
    n_req, n_steps, heads, kv_heads, groups, rows_c, hd, exp_scale = dims
    rows_q = n_steps * heads
    new_rows = n_steps * kv_heads
    blk = order_ref[pl.program_id(0)]

    col = lax.broadcasted_iota(jnp.int32, (rows_q, rows_c), 1)
    row = lax.broadcasted_iota(jnp.int32, (rows_q, rows_c), 0)
    same_head = (col % kv_heads) == ((row % heads) // groups)
    lag = jnp.where(same_head, col // kv_heads - row // heads, jnp.int32(1 << 30))
    win_row = lax.broadcasted_iota(jnp.int32, (2 * new_rows, hd), 0)
    ml_lane = lax.broadcasted_iota(jnp.int32, (rows_q, 2 * rows_q), 1)
    ml_row = lax.broadcasted_iota(jnp.int32, (rows_q, 2 * rows_q), 0)
    pad = jnp.zeros((new_rows, hd), jnp.float32)

    for j in range(n_req):
        rel = rel_ref[blk * n_req + j]
        first = rel * kv_heads
        base = pl.multiple_of(jnp.clip((first >> 4) << 4, 0, rows_c - 2 * new_rows), 16)
        off = first - base
        inside = (win_row >= off) & (win_row < off + new_rows)
        for src, new, dst in ((k_ref, kn_ref, ko_ref), (v_ref, vn_ref, vo_ref)):
            dst[j] = src[j]
            rolled = pltpu.roll(jnp.concatenate([new[j].astype(jnp.float32), pad], axis=0), off & (2 * new_rows - 1), 0)
            window = src[j, pl.ds(base, 2 * new_rows), :].astype(jnp.float32)
            dst[j, pl.ds(base, 2 * new_rows), :] = jnp.where(inside, rolled, window).astype(dst.dtype)
        query = q_ref[:, j].reshape(rows_q, hd)
        scores = lax.dot_general(query, ko_ref[j], (((1,), (1,)), ((), ())), preferred_element_type=jnp.float32)
        scores = jnp.where(lag <= rel, scores, MASKED)
        top = jnp.maximum(jnp.max(scores, axis=1, keepdims=True), FLOOR)
        probs = jnp.exp2((scores - top) * exp_scale)
        total = jnp.sum(probs, axis=1, keepdims=True)
        o_ref[j] = lax.dot_general(probs.astype(jnp.bfloat16), vo_ref[j], (((1,), (0,)), ((), ())), preferred_element_type=jnp.float32)
        packed = jnp.where(ml_lane == ml_row, top, jnp.where(ml_lane == ml_row + rows_q, total, 0.0))
        ml_ref[j] = jnp.sum(packed, axis=0, keepdims=True)


def attention(order, rel, q, k_new, v_new, k_cache, v_cache, kv_heads, exp_scale, n_req=4):
    n_steps, n_batch, heads, hd = q.shape
    rows_c = k_cache.shape[1]
    new_rows = n_steps * kv_heads
    rows_q = n_steps * heads
    dims = (n_req, n_steps, heads, kv_heads, heads // kv_heads, rows_c, hd, exp_scale)
    cache_blk = pl.BlockSpec((n_req, rows_c, hd), lambda i, order, rel: (order[i], 0, 0))
    new_blk = pl.BlockSpec((n_req, new_rows, hd), lambda i, order, rel: (order[i], 0, 0))
    cache_shape = jax.ShapeDtypeStruct(k_cache.shape, k_cache.dtype)
    return pl.pallas_call(
        functools.partial(attn_kernel, dims),
        grid_spec=pltpu.PrefetchScalarGridSpec(
            num_scalar_prefetch=2,
            grid=(n_batch // n_req,),
            in_specs=[pl.BlockSpec((n_steps, n_req, heads, hd), lambda i, order, rel: (0, order[i], 0, 0)),
                      new_blk, new_blk, cache_blk, cache_blk],
            out_specs=[cache_blk, cache_blk,
                       pl.BlockSpec((n_req, rows_q, hd), lambda i, order, rel: (i, 0, 0)),
                       pl.BlockSpec((n_req, 1, 2 * rows_q), lambda i, order, rel: (i, 0, 0))],
        ),
        out_shape=[cache_shape, cache_shape,
                   jax.ShapeDtypeStruct((n_batch, rows_q, hd), jnp.float32),
                   jax.ShapeDtypeStruct((n_batch, 1, 2 * rows_q), jnp.float32)],
        compiler_params=pltpu.CompilerParams(dimension_semantics=("arbitrary",), vmem_limit_bytes=40 * 2**20),
        cost_estimate=pl.CostEstimate(flops=4 * n_batch * rows_q * rows_c * hd, bytes_accessed=8 * n_batch * rows_c * hd,
                                      transcendentals=n_batch * rows_q * rows_c),
        name="decode_attention",
    )(order, rel, q, k_new, v_new, k_cache, v_cache)


def assemble_kernel(own, cw, sp_ref, *refs):
    out_ref = refs[-1]
    sp = sp_ref[0]
    for c in range(len(refs) // 4):
        for flip in range(4):
            start = pl.multiple_of((sp ^ flip) * own, own)
            out_ref[0, pl.ds(start, own), c * cw:(c + 1) * cw] = refs[c * 4 + flip][0].astype(out_ref.dtype)


def assemble(sp, pieces):
    n_steps, own, cw = pieces[0][0].shape
    n_chunks = len(pieces)
    piece_blk = pl.BlockSpec((1, own, cw), lambda i, sp: (i, 0, 0))
    return pl.pallas_call(
        functools.partial(assemble_kernel, own, cw),
        grid_spec=pltpu.PrefetchScalarGridSpec(
            num_scalar_prefetch=1,
            grid=(n_steps,),
            in_specs=[piece_blk] * (4 * n_chunks),
            out_specs=pl.BlockSpec((1, 4 * own, cw * n_chunks), lambda i, sp: (i, 0, 0)),
        ),
        out_shape=jax.ShapeDtypeStruct((n_steps, 4 * own, cw * n_chunks), jnp.bfloat16),
        compiler_params=pltpu.CompilerParams(dimension_semantics=("arbitrary",)),
        name="assemble_hidden",
    )(sp.reshape(1), *[piece for chunk in pieces for piece in chunk])


def merge(mine, other, exp_scale):
    out_a, max_a, sum_a = mine
    out_b, max_b, sum_b = other
    top = jnp.maximum(max_a, max_b)
    wt_a = jnp.exp2((max_a - top) * exp_scale)
    wt_b = jnp.exp2((max_b - top) * exp_scale)
    return wt_a[..., None] * out_a + wt_b[..., None] * out_b, top, wt_a * sum_a + wt_b * sum_b


def solution(mesh):
    cache_spec = P('dp', 'sp', 'tp', None)
    col_spec = P(None, 'tp')
    row_spec = P('tp', None)
    in_specs = (P(None, 'dp', None), P('dp'), cache_spec, cache_spec, col_spec, col_spec, col_spec, row_spec,
                col_spec, col_spec, row_spec, P(), P(), P(), P())
    out_specs = (P(None, 'dp', None), cache_spec, cache_spec)
    core_perm = [(0, 1), (1, 0), (2, 3), (3, 2)]
    chip_perm = [(0, 2), (2, 0), (1, 3), (3, 1)]
    tp_perm = [(0, 1), (1, 0)]

    def shard_body(hidden, start_pos, k_cache, v_cache, w_q, w_k, w_v, w_o, w_gate, w_up, w_down, attn_norm, mlp_norm, q_gain, k_gain):
        n_steps, n_batch, width = hidden.shape
        seq_blk, kv_heads, hd = k_cache.shape[1], k_cache.shape[2], k_cache.shape[3]
        heads = w_q.shape[1] // hd
        rows_q = n_steps * heads
        exp_scale = hd ** -0.5 * math.log2(math.e)
        sp = lax.axis_index('sp')
        core, chip = sp % 2, sp // 2
        own = n_batch // 4

        tok_pos = start_pos[None, :] + jnp.arange(n_steps, dtype=jnp.int32)[:, None]
        normed = rms_scale(hidden, attn_norm).astype(jnp.bfloat16).reshape(n_steps * n_batch, width)
        q_raw = jnp.dot(normed, w_q, preferred_element_type=jnp.float32).reshape(n_steps, n_batch, heads, hd)
        k_raw = jnp.dot(normed, w_k, preferred_element_type=jnp.float32).reshape(n_steps, n_batch, kv_heads, hd)
        v_new = jnp.dot(normed, w_v, preferred_element_type=jnp.float32).astype(jnp.bfloat16).reshape(n_steps, n_batch, kv_heads, hd)
        q_rot = apply_rope(rms_scale(q_raw, q_gain), tok_pos).astype(jnp.bfloat16)
        k_new = apply_rope(rms_scale(k_raw, k_gain), tok_pos).astype(jnp.bfloat16)
        k_rows = k_new.transpose(1, 0, 2, 3).reshape(n_batch, n_steps * kv_heads, hd)
        v_rows = v_new.transpose(1, 0, 2, 3).reshape(n_batch, n_steps * kv_heads, hd)

        n_req = 4
        per = own // n_req
        part = jnp.stack([(1 - chip) * 2 + (1 - core), chip * 2 + (1 - core), (1 - chip) * 2 + core, chip * 2 + core])
        order = (part[:, None] * per + jnp.arange(per)[None, :]).reshape(-1).astype(jnp.int32)
        rel = start_pos - sp * seq_blk
        flat = (n_batch, seq_blk * kv_heads, hd)
        k_out, v_out, o_part, ml = attention(order, rel, q_rot, k_rows, v_rows, k_cache.reshape(flat), v_cache.reshape(flat),
                                             kv_heads, exp_scale, n_req)

        half = n_batch // 2
        ml = ml.reshape(n_batch, 2 * rows_q)
        o_recv = lax.ppermute(o_part[:half], 'sp', core_perm)
        ml_recv = lax.ppermute(ml[:half], 'sp', core_perm)
        both = merge((o_part[half:], ml[half:, :rows_q], ml[half:, rows_q:]),
                     (o_recv, ml_recv[:, :rows_q], ml_recv[:, rows_q:]), exp_scale)
        far = [lax.ppermute(part_[:own], 'sp', chip_perm) for part_ in both]
        o_sum, _, l_sum = merge([part_[own:] for part_ in both], far, exp_scale)
        attn_in = (o_sum / l_sum[..., None]).astype(jnp.bfloat16).reshape(own, n_steps, heads * hd)
        attn_in = attn_in.transpose(1, 0, 2).reshape(n_steps * own, heads * hd)

        x_own = lax.dynamic_slice_in_dim(hidden, sp * own, own, axis=1).reshape(n_steps * own, width)
        o_mine = jnp.dot(attn_in, w_o, preferred_element_type=jnp.float32)
        attn_out = o_mine + lax.ppermute(o_mine, 'tp', tp_perm)
        residual = (x_own.astype(jnp.float32) + attn_out).astype(jnp.bfloat16)
        mlp_in = rms_scale(residual, mlp_norm).astype(jnp.bfloat16)
        gate_act = jnp.dot(mlp_in, w_gate, preferred_element_type=jnp.float32)
        up_proj = jnp.dot(mlp_in, w_up, preferred_element_type=jnp.float32)
        mlp_act = (jax.nn.silu(gate_act) * up_proj).astype(jnp.bfloat16)
        n_chunks = 4
        cw = width // n_chunks
        pieces = []
        for c in range(n_chunks):
            sl = slice(c * cw, (c + 1) * cw)
            mine = jnp.dot(mlp_act, w_down[:, sl], preferred_element_type=jnp.float32)
            mine = residual[:, sl].astype(jnp.float32) + (mine + lax.ppermute(mine, 'tp', tp_perm))
            near = lax.ppermute(mine, 'sp', core_perm)
            across = lax.ppermute(mine, 'sp', chip_perm)
            diag = lax.ppermute(across, 'sp', core_perm)
            pieces.append([piece.reshape(n_steps, own, cw) for piece in (mine, near, across, diag)])
        hid_out = assemble(sp, pieces)
        return hid_out, k_out.reshape(k_cache.shape), v_out.reshape(v_cache.shape)

    return jax.shard_map(shard_body, mesh=mesh, in_specs=in_specs, out_specs=out_specs, check_vma=False)
```

```python
import functools
import math

import jax
import jax.numpy as jnp
from jax import lax
from jax.experimental import pallas as pl
from jax.experimental.pallas import tpu as pltpu
from jax.sharding import PartitionSpec as P

ROPE_BASE = 1000000.0
NORM_EPS = 1e-06
MASKED = -3e38
FLOOR = -1e38


def rms_scale(values, gain_vec):
    wide_vals = values.astype(jnp.float32)
    inv_rms = lax.rsqrt(jnp.mean(wide_vals * wide_vals, axis=-1, keepdims=True) + NORM_EPS)
    return wide_vals * inv_rms * gain_vec.astype(jnp.float32)


def rope_tables(tok_pos, head_dim):
    half_dim = head_dim // 2
    freqs = ROPE_BASE ** (-(jnp.arange(half_dim, dtype=jnp.float32) * (2.0 / head_dim)))
    angles = tok_pos.astype(jnp.float32)[:, None] * freqs[None, :]
    cos_tab = jnp.cos(angles)
    sin_tab = jnp.sin(angles)
    return jnp.concatenate([cos_tab, cos_tab], axis=-1), jnp.concatenate([-sin_tab, sin_tab], axis=-1)


def qkv_kernel(dims, x_ref, norm_ref, cos_ref, sin_ref, qg_ref, kg_ref, wq_hbm, wk_hbm, wv_hbm, q_ref, k_ref, v_ref,
               n_ref, y_ref, qf_ref, wbuf, sems):
    heads, kv_heads, hd, unit, n_buf = dims
    tokens = x_ref.shape[0]
    rows_blk = 64
    per = unit // hd
    n_q, n_kv = heads // per, kv_heads // per
    total = n_q + 2 * n_kv

    def fetch(hbm, col, slot):
        return pltpu.make_async_copy(hbm.at[:, pl.ds(pl.multiple_of(col * unit, unit), unit)], wbuf.at[slot], sems.at[slot])

    def start(g):
        slot = lax.rem(g, n_buf)

        @pl.when(g < n_q)
        def _():
            fetch(wq_hbm, g, slot).start()

        @pl.when((g >= n_q) & (g < n_q + n_kv))
        def _():
            fetch(wk_hbm, g - n_q, slot).start()

        @pl.when((g >= n_q + n_kv) & (g < total))
        def _():
            fetch(wv_hbm, g - n_q - n_kv, slot).start()

    for g in range(n_buf - 1):
        start(jnp.int32(g))

    def norm_rows(i, carry):
        rows = pl.ds(pl.multiple_of(i * rows_blk, rows_blk), rows_blk)
        wide = x_ref[rows, :].astype(jnp.float32)
        inv = lax.rsqrt(jnp.mean(wide * wide, axis=-1, keepdims=True) + NORM_EPS)
        n_ref[rows, :] = (wide * inv * norm_ref[...].astype(jnp.float32)).astype(n_ref.dtype)
        return carry

    lax.fori_loop(0, tokens // rows_blk, norm_rows, 0)

    def project(g):
        slot = lax.rem(g, n_buf)
        start(g + n_buf - 1)
        fetch(wq_hbm, 0, slot).wait()
        y_ref[...] = jnp.dot(n_ref[...], wbuf[slot], preferred_element_type=jnp.float32)

    def rotate(vec, gain_ref):
        inv = lax.rsqrt(jnp.mean(vec * vec, axis=-1, keepdims=True) + NORM_EPS)
        vec = vec * inv * gain_ref[...].astype(jnp.float32)
        return vec * cos_ref[...] + pltpu.roll(vec, hd // 2, 1) * sin_ref[...]

    def q_unit(g, carry):
        project(g)
        for h in range(per):
            qf_ref[pl.ds(g * per + h, tokens, stride=heads), :] = rotate(y_ref[:, h * hd:(h + 1) * hd], qg_ref)
        return carry

    lax.fori_loop(0, n_q, q_unit, 0)

    def k_unit(g, carry):
        project(n_q + g)
        for h in range(per):
            row = rotate(y_ref[:, h * hd:(h + 1) * hd], kg_ref).astype(jnp.bfloat16)
            k_ref[pl.ds(g * per + h, tokens, stride=kv_heads), :] = row.astype(jnp.float32)
        return carry

    lax.fori_loop(0, n_kv, k_unit, 0)

    def v_unit(g, carry):
        project(n_q + n_kv + g)
        for h in range(per):
            row = y_ref[:, h * hd:(h + 1) * hd].astype(jnp.bfloat16)
            v_ref[pl.ds(g * per + h, tokens, stride=kv_heads), :] = row.astype(jnp.float32)
        return carry

    lax.fori_loop(0, n_kv, v_unit, 0)

    def cast_rows(i, carry):
        rows = pl.ds(pl.multiple_of(i * 512, 512), 512)
        q_ref[rows, :] = qf_ref[rows, :].astype(q_ref.dtype)
        return carry

    lax.fori_loop(0, tokens * heads // 512, cast_rows, 0)


def project_qkv(x, norm, cos_tab, sin_tab, q_gain, k_gain, w_q, w_k, w_v):
    tokens, width = x.shape
    hd = q_gain.shape[0]
    heads, kv_heads = w_q.shape[1] // hd, w_k.shape[1] // hd
    unit, n_buf = 2 * hd, 4
    vmem = pl.BlockSpec(memory_space=pltpu.VMEM)
    hbm = pl.BlockSpec(memory_space=pl.ANY)
    cols = (heads + 2 * kv_heads) * hd
    return pl.pallas_call(
        functools.partial(qkv_kernel, (heads, kv_heads, hd, unit, n_buf)),
        in_specs=[vmem] * 6 + [hbm] * 3,
        out_specs=[vmem] * 3,
        out_shape=[jax.ShapeDtypeStruct((tokens * heads, hd), jnp.bfloat16),
                   jax.ShapeDtypeStruct((tokens * kv_heads, hd), jnp.float32),
                   jax.ShapeDtypeStruct((tokens * kv_heads, hd), jnp.float32)],
        scratch_shapes=[pltpu.VMEM((tokens, width), jnp.bfloat16),
                        pltpu.VMEM((tokens, unit), jnp.float32),
                        pltpu.VMEM((tokens * heads, hd), jnp.float32),
                        pltpu.VMEM((n_buf, width, unit), jnp.bfloat16),
                        pltpu.SemaphoreType.DMA((n_buf,))],
        compiler_params=pltpu.CompilerParams(vmem_limit_bytes=48 * 2**20),
        cost_estimate=pl.CostEstimate(flops=2 * tokens * width * cols, bytes_accessed=2 * width * cols, transcendentals=0),
        name="project_qkv",
    )(x, norm.reshape(1, width), cos_tab, sin_tab, q_gain.reshape(1, hd), k_gain.reshape(1, hd), w_q, w_k, w_v)


def attn_kernel(dims, order_ref, rel_ref, q_ref, kn_ref, vn_ref, k_ref, v_ref, ko_ref, vo_ref, o_ref, ml_ref):
    n_req, n_steps, heads, kv_heads, groups, rows_c, hd, exp_scale = dims
    rows_q = n_steps * heads
    new_rows = n_steps * kv_heads
    blk = order_ref[pl.program_id(0)]

    col = lax.broadcasted_iota(jnp.int32, (rows_q, rows_c), 1)
    row = lax.broadcasted_iota(jnp.int32, (rows_q, rows_c), 0)
    same_head = (col % kv_heads) == ((row % heads) // groups)
    lag = jnp.where(same_head, col // kv_heads - row // heads, jnp.int32(1 << 30))
    win_row = lax.broadcasted_iota(jnp.int32, (2 * new_rows, hd), 0)
    ml_lane = lax.broadcasted_iota(jnp.int32, (rows_q, 2 * rows_q), 1)
    ml_row = lax.broadcasted_iota(jnp.int32, (rows_q, 2 * rows_q), 0)
    pad = jnp.zeros((new_rows, hd), jnp.float32)

    for j in range(n_req):
        rel = rel_ref[blk * n_req + j]
        first = rel * kv_heads
        base = pl.multiple_of(jnp.clip((first >> 4) << 4, 0, rows_c - 2 * new_rows), 16)
        off = first - base
        inside = (win_row >= off) & (win_row < off + new_rows)
        for src, new, dst in ((k_ref, kn_ref, ko_ref), (v_ref, vn_ref, vo_ref)):
            dst[j] = src[j]
            fresh = [new[t, j * kv_heads:(j + 1) * kv_heads, :] for t in range(n_steps)]
            rolled = pltpu.roll(jnp.concatenate(fresh + [pad], axis=0), off & (2 * new_rows - 1), 0)
            window = src[j, pl.ds(base, 2 * new_rows), :].astype(jnp.float32)
            dst[j, pl.ds(base, 2 * new_rows), :] = jnp.where(inside, rolled, window).astype(dst.dtype)
        query = q_ref[:, j].reshape(rows_q, hd)
        scores = lax.dot_general(query, ko_ref[j], (((1,), (1,)), ((), ())), preferred_element_type=jnp.float32)
        scores = jnp.where(lag <= rel, scores, MASKED)
        top = jnp.maximum(jnp.max(scores, axis=1, keepdims=True), FLOOR)
        probs = jnp.exp2((scores - top) * exp_scale)
        total = jnp.sum(probs, axis=1, keepdims=True)
        o_ref[j] = lax.dot_general(probs.astype(jnp.bfloat16), vo_ref[j], (((1,), (0,)), ((), ())), preferred_element_type=jnp.float32)
        packed = jnp.where(ml_lane == ml_row, top, jnp.where(ml_lane == ml_row + rows_q, total, 0.0))
        ml_ref[j] = jnp.sum(packed, axis=0, keepdims=True)


def attention(order, rel, q, k_new, v_new, k_cache, v_cache, kv_heads, exp_scale, n_req=4):
    n_steps, n_batch, heads, hd = q.shape
    rows_c = k_cache.shape[1]
    rows_q = n_steps * heads
    dims = (n_req, n_steps, heads, kv_heads, heads // kv_heads, rows_c, hd, exp_scale)
    cache_blk = pl.BlockSpec((n_req, rows_c, hd), lambda i, order, rel: (order[i], 0, 0))
    new_blk = pl.BlockSpec((n_steps, n_req * kv_heads, hd), lambda i, order, rel: (0, order[i], 0))
    cache_shape = jax.ShapeDtypeStruct(k_cache.shape, k_cache.dtype)
    return pl.pallas_call(
        functools.partial(attn_kernel, dims),
        grid_spec=pltpu.PrefetchScalarGridSpec(
            num_scalar_prefetch=2,
            grid=(n_batch // n_req,),
            in_specs=[pl.BlockSpec((n_steps, n_req, heads, hd), lambda i, order, rel: (0, order[i], 0, 0)),
                      new_blk, new_blk, cache_blk, cache_blk],
            out_specs=[cache_blk, cache_blk,
                       pl.BlockSpec((n_req, rows_q, hd), lambda i, order, rel: (i, 0, 0)),
                       pl.BlockSpec((n_req, 1, 2 * rows_q), lambda i, order, rel: (i, 0, 0))],
        ),
        out_shape=[cache_shape, cache_shape,
                   jax.ShapeDtypeStruct((n_batch, rows_q, hd), jnp.float32),
                   jax.ShapeDtypeStruct((n_batch, 1, 2 * rows_q), jnp.float32)],
        compiler_params=pltpu.CompilerParams(dimension_semantics=("arbitrary",), vmem_limit_bytes=40 * 2**20),
        cost_estimate=pl.CostEstimate(flops=4 * n_batch * rows_q * rows_c * hd, bytes_accessed=8 * n_batch * rows_c * hd,
                                      transcendentals=n_batch * rows_q * rows_c),
        name="decode_attention",
    )(order, rel, q, k_new, v_new, k_cache, v_cache)


def assemble_kernel(own, cw, sp_ref, *refs):
    out_ref = refs[-1]
    sp = sp_ref[0]
    for c in range(len(refs) // 4):
        for flip in range(4):
            start = pl.multiple_of((sp ^ flip) * own, own)
            out_ref[0, pl.ds(start, own), c * cw:(c + 1) * cw] = refs[c * 4 + flip][0].astype(out_ref.dtype)


def assemble(sp, pieces):
    n_steps, own, cw = pieces[0][0].shape
    n_chunks = len(pieces)
    piece_blk = pl.BlockSpec((1, own, cw), lambda i, sp: (i, 0, 0))
    return pl.pallas_call(
        functools.partial(assemble_kernel, own, cw),
        grid_spec=pltpu.PrefetchScalarGridSpec(
            num_scalar_prefetch=1,
            grid=(n_steps,),
            in_specs=[piece_blk] * (4 * n_chunks),
            out_specs=pl.BlockSpec((1, 4 * own, cw * n_chunks), lambda i, sp: (i, 0, 0)),
        ),
        out_shape=jax.ShapeDtypeStruct((n_steps, 4 * own, cw * n_chunks), jnp.bfloat16),
        compiler_params=pltpu.CompilerParams(dimension_semantics=("arbitrary",)),
        name="assemble_hidden",
    )(sp.reshape(1), *[piece for chunk in pieces for piece in chunk])


def merge(mine, other, exp_scale):
    out_a, max_a, sum_a = mine
    out_b, max_b, sum_b = other
    top = jnp.maximum(max_a, max_b)
    wt_a = jnp.exp2((max_a - top) * exp_scale)
    wt_b = jnp.exp2((max_b - top) * exp_scale)
    return wt_a[..., None] * out_a + wt_b[..., None] * out_b, top, wt_a * sum_a + wt_b * sum_b


def solution(mesh):
    cache_spec = P('dp', 'sp', 'tp', None)
    col_spec = P(None, 'tp')
    row_spec = P('tp', None)
    in_specs = (P(None, 'dp', None), P('dp'), cache_spec, cache_spec, col_spec, col_spec, col_spec, row_spec,
                col_spec, col_spec, row_spec, P(), P(), P(), P())
    out_specs = (P(None, 'dp', None), cache_spec, cache_spec)
    core_perm = [(0, 1), (1, 0), (2, 3), (3, 2)]
    chip_perm = [(0, 2), (2, 0), (1, 3), (3, 1)]
    tp_perm = [(0, 1), (1, 0)]

    def shard_body(hidden, start_pos, k_cache, v_cache, w_q, w_k, w_v, w_o, w_gate, w_up, w_down, attn_norm, mlp_norm, q_gain, k_gain):
        n_steps, n_batch, width = hidden.shape
        seq_blk, kv_heads, hd = k_cache.shape[1], k_cache.shape[2], k_cache.shape[3]
        heads = w_q.shape[1] // hd
        rows_q = n_steps * heads
        exp_scale = hd ** -0.5 * math.log2(math.e)
        sp = lax.axis_index('sp')
        core, chip = sp % 2, sp // 2
        own = n_batch // 4

        tok_pos = (start_pos[None, :] + jnp.arange(n_steps, dtype=jnp.int32)[:, None]).reshape(-1)
        cos_tab, sin_tab = rope_tables(tok_pos, hd)
        q_rows, k_rows, v_rows = project_qkv(hidden.reshape(n_steps * n_batch, width), attn_norm, cos_tab, sin_tab,
                                             q_gain, k_gain, w_q, w_k, w_v)
        q_rot = q_rows.reshape(n_steps, n_batch, heads, hd)
        k_rows = k_rows.reshape(n_steps, n_batch * kv_heads, hd)
        v_rows = v_rows.reshape(n_steps, n_batch * kv_heads, hd)

        n_req = 4
        per = own // n_req
        part = jnp.stack([(1 - chip) * 2 + (1 - core), chip * 2 + (1 - core), (1 - chip) * 2 + core, chip * 2 + core])
        order = (part[:, None] * per + jnp.arange(per)[None, :]).reshape(-1).astype(jnp.int32)
        rel = start_pos - sp * seq_blk
        flat = (n_batch, seq_blk * kv_heads, hd)
        k_out, v_out, o_part, ml = attention(order, rel, q_rot, k_rows, v_rows, k_cache.reshape(flat), v_cache.reshape(flat),
                                             kv_heads, exp_scale, n_req)

        half = n_batch // 2
        ml = ml.reshape(n_batch, 2 * rows_q)
        o_recv = lax.ppermute(o_part[:half], 'sp', core_perm)
        ml_recv = lax.ppermute(ml[:half], 'sp', core_perm)
        both = merge((o_part[half:], ml[half:, :rows_q], ml[half:, rows_q:]),
                     (o_recv, ml_recv[:, :rows_q], ml_recv[:, rows_q:]), exp_scale)
        far = [lax.ppermute(part_[:own], 'sp', chip_perm) for part_ in both]
        o_sum, _, l_sum = merge([part_[own:] for part_ in both], far, exp_scale)
        attn_in = (o_sum / l_sum[..., None]).astype(jnp.bfloat16).reshape(own, n_steps, heads * hd)
        attn_in = attn_in.transpose(1, 0, 2).reshape(n_steps * own, heads * hd)

        x_own = lax.dynamic_slice_in_dim(hidden, sp * own, own, axis=1).reshape(n_steps * own, width)
        o_mine = jnp.dot(attn_in, w_o, preferred_element_type=jnp.float32)
        attn_out = o_mine + lax.ppermute(o_mine, 'tp', tp_perm)
        residual = (x_own.astype(jnp.float32) + attn_out).astype(jnp.bfloat16)
        mlp_in = rms_scale(residual, mlp_norm).astype(jnp.bfloat16)
        gate_act = jnp.dot(mlp_in, w_gate, preferred_element_type=jnp.float32)
        up_proj = jnp.dot(mlp_in, w_up, preferred_element_type=jnp.float32)
        mlp_act = (jax.nn.silu(gate_act) * up_proj).astype(jnp.bfloat16)
        n_chunks = 4
        cw = width // n_chunks
        pieces = []
        for c in range(n_chunks):
            sl = slice(c * cw, (c + 1) * cw)
            mine = jnp.dot(mlp_act, w_down[:, sl], preferred_element_type=jnp.float32)
            mine = residual[:, sl].astype(jnp.float32) + (mine + lax.ppermute(mine, 'tp', tp_perm))
            near = lax.ppermute(mine, 'sp', core_perm)
            across = lax.ppermute(mine, 'sp', chip_perm)
            diag = lax.ppermute(across, 'sp', core_perm)
            pieces.append([piece.reshape(n_steps, own, cw) for piece in (mine, near, across, diag)])
        hid_out = assemble(sp, pieces)
        return hid_out, k_out.reshape(k_cache.shape), v_out.reshape(v_cache.shape)

    return jax.shard_map(shard_body, mesh=mesh, in_specs=in_specs, out_specs=out_specs, check_vma=False)
```

```python
import functools
import math

import jax
import jax.numpy as jnp
from jax import lax
from jax.experimental import pallas as pl
from jax.experimental.pallas import tpu as pltpu
from jax.sharding import PartitionSpec as P

ROPE_BASE = 1000000.0
NORM_EPS = 1e-06
MASKED = -3e38
FLOOR = -1e38


def rms_scale(values, gain_vec):
    wide_vals = values.astype(jnp.float32)
    inv_rms = lax.rsqrt(jnp.mean(wide_vals * wide_vals, axis=-1, keepdims=True) + NORM_EPS)
    return wide_vals * inv_rms * gain_vec.astype(jnp.float32)


def rope_tables(tok_pos, head_dim):
    half_dim = head_dim // 2
    freqs = ROPE_BASE ** (-(jnp.arange(half_dim, dtype=jnp.float32) * (2.0 / head_dim)))
    angles = tok_pos.astype(jnp.float32)[:, None] * freqs[None, :]
    cos_tab = jnp.cos(angles)
    sin_tab = jnp.sin(angles)
    return jnp.concatenate([cos_tab, cos_tab], axis=-1), jnp.concatenate([-sin_tab, sin_tab], axis=-1)


def qkv_kernel(dims, x_ref, norm_ref, cos_ref, sin_ref, qg_ref, kg_ref, wq_hbm, wk_hbm, wv_hbm, q_ref, k_ref, v_ref,
               n_ref, y_ref, qf_ref, wbuf, sems):
    heads, kv_heads, hd, unit, n_buf = dims
    tokens = x_ref.shape[0]
    rows_blk = 64
    per = unit // hd
    n_q, n_kv = heads // per, kv_heads // per
    total = n_q + 2 * n_kv

    def fetch(hbm, col, slot):
        return pltpu.make_async_copy(hbm.at[:, pl.ds(pl.multiple_of(col * unit, unit), unit)], wbuf.at[slot], sems.at[slot])

    def start(g):
        slot = lax.rem(g, n_buf)

        @pl.when(g < n_q)
        def _():
            fetch(wq_hbm, g, slot).start()

        @pl.when((g >= n_q) & (g < n_q + n_kv))
        def _():
            fetch(wk_hbm, g - n_q, slot).start()

        @pl.when((g >= n_q + n_kv) & (g < total))
        def _():
            fetch(wv_hbm, g - n_q - n_kv, slot).start()

    for g in range(n_buf - 1):
        start(jnp.int32(g))

    def norm_rows(i, carry):
        rows = pl.ds(pl.multiple_of(i * rows_blk, rows_blk), rows_blk)
        wide = x_ref[rows, :].astype(jnp.float32)
        inv = lax.rsqrt(jnp.mean(wide * wide, axis=-1, keepdims=True) + NORM_EPS)
        n_ref[rows, :] = (wide * inv * norm_ref[...].astype(jnp.float32)).astype(n_ref.dtype)
        return carry

    lax.fori_loop(0, tokens // rows_blk, norm_rows, 0)

    def project(g):
        slot = lax.rem(g, n_buf)
        start(g + n_buf - 1)
        fetch(wq_hbm, 0, slot).wait()
        y_ref[...] = jnp.dot(n_ref[...], wbuf[slot], preferred_element_type=jnp.float32)

    def rotate(vec, gain_ref):
        inv = lax.rsqrt(jnp.mean(vec * vec, axis=-1, keepdims=True) + NORM_EPS)
        vec = vec * inv * gain_ref[...].astype(jnp.float32)
        return vec * cos_ref[...] + pltpu.roll(vec, hd // 2, 1) * sin_ref[...]

    def q_unit(g, carry):
        project(g)
        for h in range(per):
            qf_ref[pl.ds(g * per + h, tokens, stride=heads), :] = rotate(y_ref[:, h * hd:(h + 1) * hd], qg_ref)
        return carry

    lax.fori_loop(0, n_q, q_unit, 0)

    def k_unit(g, carry):
        project(n_q + g)
        for h in range(per):
            row = rotate(y_ref[:, h * hd:(h + 1) * hd], kg_ref).astype(jnp.bfloat16)
            k_ref[pl.ds(g * per + h, tokens, stride=kv_heads), :] = row.astype(jnp.float32)
        return carry

    lax.fori_loop(0, n_kv, k_unit, 0)

    def v_unit(g, carry):
        project(n_q + n_kv + g)
        for h in range(per):
            row = y_ref[:, h * hd:(h + 1) * hd].astype(jnp.bfloat16)
            v_ref[pl.ds(g * per + h, tokens, stride=kv_heads), :] = row.astype(jnp.float32)
        return carry

    lax.fori_loop(0, n_kv, v_unit, 0)

    def cast_rows(i, carry):
        rows = pl.ds(pl.multiple_of(i * 512, 512), 512)
        q_ref[rows, :] = qf_ref[rows, :].astype(q_ref.dtype)
        return carry

    lax.fori_loop(0, tokens * heads // 512, cast_rows, 0)


def project_qkv(x, norm, cos_tab, sin_tab, q_gain, k_gain, w_q, w_k, w_v):
    tokens, width = x.shape
    hd = q_gain.shape[0]
    heads, kv_heads = w_q.shape[1] // hd, w_k.shape[1] // hd
    unit, n_buf = 2 * hd, 4
    vmem = pl.BlockSpec(memory_space=pltpu.VMEM)
    hbm = pl.BlockSpec(memory_space=pl.ANY)
    cols = (heads + 2 * kv_heads) * hd
    return pl.pallas_call(
        functools.partial(qkv_kernel, (heads, kv_heads, hd, unit, n_buf)),
        in_specs=[vmem] * 6 + [hbm] * 3,
        out_specs=[vmem] * 3,
        out_shape=[jax.ShapeDtypeStruct((tokens * heads, hd), jnp.bfloat16),
                   jax.ShapeDtypeStruct((tokens * kv_heads, hd), jnp.float32),
                   jax.ShapeDtypeStruct((tokens * kv_heads, hd), jnp.float32)],
        scratch_shapes=[pltpu.VMEM((tokens, width), jnp.bfloat16),
                        pltpu.VMEM((tokens, unit), jnp.float32),
                        pltpu.VMEM((tokens * heads, hd), jnp.float32),
                        pltpu.VMEM((n_buf, width, unit), jnp.bfloat16),
                        pltpu.SemaphoreType.DMA((n_buf,))],
        compiler_params=pltpu.CompilerParams(vmem_limit_bytes=48 * 2**20),
        cost_estimate=pl.CostEstimate(flops=2 * tokens * width * cols, bytes_accessed=2 * width * cols, transcendentals=0),
        name="project_qkv",
    )(x, norm.reshape(1, width), cos_tab, sin_tab, q_gain.reshape(1, hd), k_gain.reshape(1, hd), w_q, w_k, w_v)


def attn_kernel(dims, order_ref, rel_ref, q_ref, kn_ref, vn_ref, k_ref, v_ref, ko_ref, vo_ref, o_ref, ml_ref):
    n_req, n_steps, heads, kv_heads, groups, rows_c, hd, exp_scale = dims
    rows_q = n_steps * heads
    new_rows = n_steps * kv_heads
    blk = order_ref[pl.program_id(0)]

    col = lax.broadcasted_iota(jnp.int32, (rows_q, rows_c), 1)
    row = lax.broadcasted_iota(jnp.int32, (rows_q, rows_c), 0)
    same_head = (col % kv_heads) == ((row % heads) // groups)
    lag = jnp.where(same_head, col // kv_heads - row // heads, jnp.int32(1 << 30))
    win_row = lax.broadcasted_iota(jnp.int32, (2 * new_rows, hd), 0)
    ml_lane = lax.broadcasted_iota(jnp.int32, (rows_q, 2 * rows_q), 1)
    ml_row = lax.broadcasted_iota(jnp.int32, (rows_q, 2 * rows_q), 0)
    pad = jnp.zeros((new_rows, hd), jnp.float32)

    for j in range(n_req):
        rel = rel_ref[blk * n_req + j]
        first = rel * kv_heads
        base = pl.multiple_of(jnp.clip((first >> 4) << 4, 0, rows_c - 2 * new_rows), 16)
        off = first - base
        inside = (win_row >= off) & (win_row < off + new_rows)
        for src, new, dst in ((k_ref, kn_ref, ko_ref), (v_ref, vn_ref, vo_ref)):
            dst[j] = src[j]
            fresh = [new[t, j * kv_heads:(j + 1) * kv_heads, :] for t in range(n_steps)]
            rolled = pltpu.roll(jnp.concatenate(fresh + [pad], axis=0), off & (2 * new_rows - 1), 0)
            window = src[j, pl.ds(base, 2 * new_rows), :].astype(jnp.float32)
            dst[j, pl.ds(base, 2 * new_rows), :] = jnp.where(inside, rolled, window).astype(dst.dtype)
        query = q_ref[:, j].reshape(rows_q, hd)
        scores = lax.dot_general(query, ko_ref[j], (((1,), (1,)), ((), ())), preferred_element_type=jnp.float32)
        scores = jnp.where(lag <= rel, scores, MASKED)
        top = jnp.maximum(jnp.max(scores, axis=1, keepdims=True), FLOOR)
        probs = jnp.exp2((scores - top) * exp_scale)
        total = jnp.sum(probs, axis=1, keepdims=True)
        o_ref[j] = lax.dot_general(probs.astype(jnp.bfloat16), vo_ref[j], (((1,), (0,)), ((), ())), preferred_element_type=jnp.float32)
        packed = jnp.where(ml_lane == ml_row, top, jnp.where(ml_lane == ml_row + rows_q, total, 0.0))
        ml_ref[j] = jnp.sum(packed, axis=0, keepdims=True)


def attention(order, rel, q, k_new, v_new, k_cache, v_cache, kv_heads, exp_scale, n_req=4):
    n_steps, n_batch, heads, hd = q.shape
    rows_c = k_cache.shape[1]
    rows_q = n_steps * heads
    dims = (n_req, n_steps, heads, kv_heads, heads // kv_heads, rows_c, hd, exp_scale)
    cache_blk = pl.BlockSpec((n_req, rows_c, hd), lambda i, order, rel: (order[i], 0, 0))
    new_blk = pl.BlockSpec((n_steps, n_req * kv_heads, hd), lambda i, order, rel: (0, order[i], 0))
    cache_shape = jax.ShapeDtypeStruct(k_cache.shape, k_cache.dtype)
    return pl.pallas_call(
        functools.partial(attn_kernel, dims),
        grid_spec=pltpu.PrefetchScalarGridSpec(
            num_scalar_prefetch=2,
            grid=(n_batch // n_req,),
            in_specs=[pl.BlockSpec((n_steps, n_req, heads, hd), lambda i, order, rel: (0, order[i], 0, 0)),
                      new_blk, new_blk, cache_blk, cache_blk],
            out_specs=[cache_blk, cache_blk,
                       pl.BlockSpec((n_req, rows_q, hd), lambda i, order, rel: (i, 0, 0)),
                       pl.BlockSpec((n_req, 1, 2 * rows_q), lambda i, order, rel: (i, 0, 0))],
        ),
        out_shape=[cache_shape, cache_shape,
                   jax.ShapeDtypeStruct((n_batch, rows_q, hd), jnp.float32),
                   jax.ShapeDtypeStruct((n_batch, 1, 2 * rows_q), jnp.float32)],
        compiler_params=pltpu.CompilerParams(dimension_semantics=("arbitrary",), vmem_limit_bytes=40 * 2**20),
        cost_estimate=pl.CostEstimate(flops=4 * n_batch * rows_q * rows_c * hd, bytes_accessed=8 * n_batch * rows_c * hd,
                                      transcendentals=n_batch * rows_q * rows_c),
        name="decode_attention",
    )(order, rel, q, k_new, v_new, k_cache, v_cache)


def tail_kernel(dims, o_ref, ml_ref, x_ref, gain_ref, wo_hbm, wg_hbm, wu_hbm, wd_hbm, out_ref,
                ring, near1, nml, far1, fml, wts, comb, attn, part_o, recv_o, res, mid, act, part_d, recv_d, fin, across, near, diag,
                ring_sem, n1s, n1r, nms, nmr, f1s, f1r, fms, fmr, os_, or_, ds_, dr_, xs_, xr_, cs_, cr_, gs_, gr_):
    n_steps, heads, hd, n_chunks, exp_scale, n_slots = dims
    rows_q = n_steps * heads
    own = far1.shape[0]
    per = own // n_chunks
    tok = per * n_steps
    width = x_ref.shape[1]
    kt, nt = ring.shape[1], ring.shape[2]
    n_o = width // nt
    n_up = act.shape[1] // nt
    k_up, k_dn = width // kt, act.shape[1] // kt
    n_dn = width // nt
    first_up = n_o
    first_dn = n_o + 2 * k_up * n_up
    n_loads = first_dn + k_dn * n_dn

    sp = lax.axis_index('sp')
    tp = lax.axis_index('tp')
    sp_core = sp + 1 - 2 * lax.rem(sp, 2)
    sp_chip = lax.rem(sp + 2, 4)
    sp_diag = lax.rem(sp_core + 2, 4)
    to_core = {'sp': sp_core}
    to_chip = {'sp': sp_chip}
    to_tp = {'tp': 1 - tp}

    def send(src, dst, s_sem, r_sem, dev):
        return pltpu.make_async_remote_copy(src_ref=src, dst_ref=dst, send_sem=s_sem, recv_sem=r_sem, device_id=dev,
                                            device_id_type=pl.DeviceIdType.MESH)

    barrier = pltpu.get_barrier_semaphore()
    for dev in (to_core, to_chip, to_tp):
        pl.semaphore_signal(barrier, inc=1, device_id=dev, device_id_type=pl.DeviceIdType.MESH)
    pl.semaphore_wait(barrier, 3)

    near_ml = send(ml_ref.at[pl.ds(0, 2 * own)], nml, nms.at[0], nmr.at[0], to_core)
    near_ml.start()
    near_o = []
    for piece in (0, 1):
        for j in range(n_chunks):
            rows = pl.ds(piece * own + j * per, per)
            near_o.append(send(o_ref.at[rows], near1.at[rows], n1s.at[piece * n_chunks + j], n1r.at[piece * n_chunks + j], to_core))
    for copy in near_o:
        copy.start()

    def load(src, row, col, slot):
        return pltpu.make_async_copy(src.at[pl.ds(pl.multiple_of(row * kt, kt), kt), pl.ds(pl.multiple_of(col * nt, nt), nt)],
                                     ring.at[slot], ring_sem.at[slot])

    def start(idx):
        slot = lax.rem(idx, n_slots)

        @pl.when(idx < first_up)
        def _():
            load(wo_hbm, 0, idx, slot).start()

        up = idx - first_up
        sub = lax.rem(up + 2 * k_up, 2 * k_up)
        col = (up - sub) // (2 * k_up)

        @pl.when((idx >= first_up) & (idx < first_dn) & (sub < k_up))
        def _():
            load(wg_hbm, sub, col, slot).start()

        @pl.when((idx >= first_up) & (idx < first_dn) & (sub >= k_up))
        def _():
            load(wu_hbm, sub - k_up, col, slot).start()

        dn = idx - first_dn
        dsub = lax.rem(dn, k_dn)

        @pl.when((idx >= first_dn) & (idx < n_loads))
        def _():
            load(wd_hbm, dsub, (dn - dsub) // k_dn, slot).start()

    def arrived(idx):
        slot = lax.rem(idx, n_slots)
        load(wo_hbm, 0, 0, slot).wait()
        return slot

    def start_many(lo, hi):
        def one(i, carry):
            start(i)
            return carry
        lax.fori_loop(lo, hi, one, 0)

    start_many(0, n_slots)

    diag_mask = lax.broadcasted_iota(jnp.int32, (rows_q, 2 * rows_q), 0) == lax.broadcasted_iota(jnp.int32, (rows_q, 2 * rows_q), 1)
    left = lax.broadcasted_iota(jnp.int32, (per, 2 * rows_q), 1) < rows_q

    def column(row):
        return jnp.sum(jnp.where(diag_mask, row, 0.0), axis=1, keepdims=True)

    def weights(stat_a, stat_b):
        top = jnp.maximum(stat_a, stat_b)
        wt_a = jnp.exp2((stat_a - top) * exp_scale)
        wt_b = jnp.exp2((stat_b - top) * exp_scale)
        total = pltpu.roll(wt_a, rows_q, 1) * stat_a + pltpu.roll(wt_b, rows_q, 1) * stat_b
        return wt_a, wt_b, jnp.where(left, top, total)

    def merge_near(piece, j):
        base = piece * own + j * per
        near_o[piece * n_chunks + j].wait_recv()
        wt_a, wt_b, stat = weights(nml[base:base + per, :], ml_ref[2 * own + base:2 * own + base + per, :])
        wts[0] = wt_a
        wts[1] = wt_b
        nml[base:base + per, :] = stat

        def one(i, carry):
            near1[base + i] = column(wts[0, pl.ds(i, 1), :]) * near1[base + i] + column(wts[1, pl.ds(i, 1), :]) * o_ref[2 * own + base + i]
            return carry
        lax.fori_loop(0, per, one, 0)

    near_ml.wait_recv()
    far_o, far_ml = [], []
    for j in range(n_chunks):
        rows = pl.ds(j * per, per)
        merge_near(0, j)
        far_ml.append(send(nml.at[rows], fml.at[rows], fms.at[j], fmr.at[j], to_chip))
        far_o.append(send(near1.at[rows], far1.at[rows], f1s.at[j], f1r.at[j], to_chip))
        far_ml[j].start()
        far_o[j].start()
    for j in range(n_chunks):
        merge_near(1, j)

    tp_o = []
    for j in range(n_chunks):
        base = j * per
        far_ml[j].wait_recv()
        far_o[j].wait_recv()
        wt_a, wt_b, stat = weights(nml[own + base:own + base + per, :], fml[base:base + per, :])
        inv = pltpu.roll(1.0 / stat, rows_q, 1)
        wts[0] = wt_a * inv
        wts[1] = wt_b * inv

        def one(i, carry, base=base):
            rows = pl.ds(pl.multiple_of(i * rows_q, rows_q), rows_q)
            comb[rows, :] = column(wts[0, pl.ds(i, 1), :]) * near1[own + base + i] + column(wts[1, pl.ds(i, 1), :]) * far1[base + i]
            return carry
        lax.fori_loop(0, per, one, 0)
        for step in range(n_steps):
            for h in range(heads):
                attn[step * per:(step + 1) * per, h * hd:(h + 1) * hd] = comb[pl.ds(step * heads + h, per, stride=rows_q), :]
        attn_in = attn[...].astype(jnp.bfloat16)

        def o_tile(n, carry, j=j, attn_in=attn_in):
            if j == 0:
                arrived(n)
            part_o[j, :, pl.ds(pl.multiple_of(n * nt, nt), nt)] = jnp.dot(attn_in, ring[n], preferred_element_type=jnp.float32)
            return carry
        lax.fori_loop(0, n_o, o_tile, 0)
        tp_o.append(send(part_o.at[j], recv_o.at[j], os_.at[j], or_.at[j], to_tp))
        tp_o[j].start()
    start_many(n_slots, n_slots + n_o)

    half = 16
    for j in range(n_chunks):
        tp_o[j].wait_recv()

        def norm_rows(i, carry, j=j):
            sub = pl.ds(pl.multiple_of(i * half, half), half)
            rows = pl.ds(pl.multiple_of(j * tok + i * half, half), half)
            summed = x_ref[rows, :].astype(jnp.float32) + (part_o[j, sub, :] + recv_o[j, sub, :])
            resid = summed.astype(jnp.bfloat16)
            res[rows, :] = resid
            wide = resid.astype(jnp.float32)
            inv = lax.rsqrt(jnp.mean(wide * wide, axis=-1, keepdims=True) + NORM_EPS)
            mid[rows, :] = (wide * inv * gain_ref[...].astype(jnp.float32)).astype(jnp.bfloat16)
            return carry
        lax.fori_loop(0, tok // half, norm_rows, 0)

    def up_tile(t, carry):
        idx = first_up + 2 * k_up * t
        total = []
        for side in (0, 1):
            acc = None
            for k in range(k_up):
                slot = arrived(idx + side * k_up + k)
                prod = jnp.dot(mid[:, k * kt:(k + 1) * kt], ring[slot], preferred_element_type=jnp.float32)
                acc = prod if acc is None else acc + prod
            total.append(acc)
        gate, up = total
        act[:, pl.ds(pl.multiple_of(t * nt, nt), nt)] = (jax.nn.silu(gate) * up).astype(jnp.bfloat16)
        for k in range(2 * k_up):
            start(idx + k + n_slots)
        return carry

    lax.fori_loop(0, n_up, up_tile, 0)

    tp_d, chip_d, core_d, diag_d = [], [], [], []
    for t in range(n_dn):
        tp_d.append(send(part_d.at[t], recv_d.at[t], ds_.at[t], dr_.at[t], to_tp))
        chip_d.append(send(fin.at[t], across.at[t], xs_.at[t], xr_.at[t], to_chip))
        core_d.append(send(fin.at[t], near.at[t], cs_.at[t], cr_.at[t], to_core))
        diag_d.append(send(across.at[t], diag.at[t], gs_.at[t], gr_.at[t], to_core))

    n_tok = res.shape[0]

    def emit(who, t, value):
        rows = pl.ds(pl.multiple_of(who * n_tok, n_tok), n_tok)
        out_ref[rows, t * nt:(t + 1) * nt] = value.astype(out_ref.dtype)

    def down(t):
        acc = None
        for k in range(k_dn):
            slot = arrived(first_dn + k_dn * t + k)
            prod = jnp.dot(act[:, k * kt:(k + 1) * kt], ring[slot], preferred_element_type=jnp.float32)
            acc = prod if acc is None else acc + prod
        part_d[t] = acc
        tp_d[t].start()
        for k in range(k_dn):
            start(jnp.int32(first_dn + k_dn * t + k + n_slots))

    def finish(t):
        tp_d[t].wait_recv()
        fin[t] = res[:, t * nt:(t + 1) * nt].astype(jnp.float32) + (part_d[t] + recv_d[t])
        chip_d[t].start()
        core_d[t].start()
        emit(sp, t, fin[t])

    def forward(t):
        chip_d[t].wait_recv()
        diag_d[t].start()
        emit(sp_chip, t, across[t])
        core_d[t].wait_recv()
        emit(sp_core, t, near[t])

    for t in range(n_dn):
        down(t)
        if t == 5:
            finish(0)
    for t in range(1, n_dn):
        finish(t)
        forward(t - 1)
    forward(n_dn - 1)
    for t in range(n_dn):
        diag_d[t].wait_recv()
        emit(sp_diag, t, diag[t])
    for copy in near_o + [near_ml] + far_o + far_ml + tp_o + tp_d + chip_d + core_d + diag_d:
        copy.wait_send()


def finish_layer(o_part, ml, x_own, norm, w_o, w_gate, w_up, w_down, n_steps, heads, exp_scale):
    n_batch, rows_q, hd = o_part.shape
    tokens, width = x_own.shape
    own = tokens // n_steps
    inner = w_gate.shape[1]
    n_chunks, n_slots, kt, nt = 4, 12, 2048, 512
    per = own // n_chunks
    n_dn = width // nt
    vmem = pl.BlockSpec(memory_space=pltpu.VMEM)
    hbm = pl.BlockSpec(memory_space=pl.ANY)
    f32, bf16 = jnp.float32, jnp.bfloat16
    tiles = pltpu.VMEM((n_dn, tokens, nt), f32)
    dma = pltpu.SemaphoreType.DMA
    return pl.pallas_call(
        functools.partial(tail_kernel, (n_steps, heads, hd, n_chunks, exp_scale, n_slots)),
        in_specs=[vmem] * 4 + [hbm] * 4,
        out_specs=vmem,
        out_shape=jax.ShapeDtypeStruct((4 * tokens, width), bf16),
        scratch_shapes=[pltpu.VMEM((n_slots, kt, nt), bf16),
                        pltpu.VMEM((2 * own, rows_q, hd), f32), pltpu.VMEM((2 * own, 2 * rows_q), f32),
                        pltpu.VMEM((own, rows_q, hd), f32), pltpu.VMEM((own, 2 * rows_q), f32),
                        pltpu.VMEM((2, per, 2 * rows_q), f32), pltpu.VMEM((per * rows_q, hd), f32),
                        pltpu.VMEM((per * n_steps, heads * hd), f32),
                        pltpu.VMEM((n_chunks, per * n_steps, width), f32), pltpu.VMEM((n_chunks, per * n_steps, width), f32),
                        pltpu.VMEM((tokens, width), bf16), pltpu.VMEM((tokens, width), bf16), pltpu.VMEM((tokens, inner), bf16),
                        tiles, tiles, tiles, tiles, tiles, tiles,
                        dma((n_slots,)), dma((2 * n_chunks,)), dma((2 * n_chunks,)), dma((1,)), dma((1,)),
                        dma((n_chunks,)), dma((n_chunks,)), dma((n_chunks,)), dma((n_chunks,)), dma((n_chunks,)), dma((n_chunks,)),
                        dma((n_dn,)), dma((n_dn,)), dma((n_dn,)), dma((n_dn,)), dma((n_dn,)), dma((n_dn,)), dma((n_dn,)), dma((n_dn,))],
        compiler_params=pltpu.CompilerParams(collective_id=0, has_side_effects=True, vmem_limit_bytes=63 * 2**20),
        name="finish_layer",
    )(o_part, ml, x_own, norm.reshape(1, width), w_o, w_gate, w_up, w_down)


def solution(mesh):
    cache_spec = P('dp', 'sp', 'tp', None)
    col_spec = P(None, 'tp')
    row_spec = P('tp', None)
    in_specs = (P(None, 'dp', None), P('dp'), cache_spec, cache_spec, col_spec, col_spec, col_spec, row_spec,
                col_spec, col_spec, row_spec, P(), P(), P(), P())
    out_specs = (P(None, 'dp', None), cache_spec, cache_spec)

    def shard_body(hidden, start_pos, k_cache, v_cache, w_q, w_k, w_v, w_o, w_gate, w_up, w_down, attn_norm, mlp_norm, q_gain, k_gain):
        n_steps, n_batch, width = hidden.shape
        seq_blk, kv_heads, hd = k_cache.shape[1], k_cache.shape[2], k_cache.shape[3]
        heads = w_q.shape[1] // hd
        rows_q = n_steps * heads
        exp_scale = hd ** -0.5 * math.log2(math.e)
        sp = lax.axis_index('sp')
        core, chip = sp % 2, sp // 2
        own = n_batch // 4

        tok_pos = (start_pos[None, :] + jnp.arange(n_steps, dtype=jnp.int32)[:, None]).reshape(-1)
        cos_tab, sin_tab = rope_tables(tok_pos, hd)
        q_rows, k_rows, v_rows = project_qkv(hidden.reshape(n_steps * n_batch, width), attn_norm, cos_tab, sin_tab,
                                             q_gain, k_gain, w_q, w_k, w_v)
        q_rot = q_rows.reshape(n_steps, n_batch, heads, hd)
        k_rows = k_rows.reshape(n_steps, n_batch * kv_heads, hd)
        v_rows = v_rows.reshape(n_steps, n_batch * kv_heads, hd)

        n_req = 4
        per = own // n_req
        part = jnp.stack([(1 - chip) * 2 + (1 - core), chip * 2 + (1 - core), (1 - chip) * 2 + core, chip * 2 + core])
        order = (part[:, None] * per + jnp.arange(per)[None, :]).reshape(-1).astype(jnp.int32)
        rel = start_pos - sp * seq_blk
        flat = (n_batch, seq_blk * kv_heads, hd)
        k_out, v_out, o_part, ml = attention(order, rel, q_rot, k_rows, v_rows, k_cache.reshape(flat), v_cache.reshape(flat),
                                             kv_heads, exp_scale, n_req)

        n_chunks = 4
        per_chunk = own // n_chunks
        x_own = lax.dynamic_slice_in_dim(hidden, sp * own, own, axis=1).reshape(n_steps, n_chunks, per_chunk, width)
        x_own = x_own.transpose(1, 0, 2, 3).reshape(n_steps * own, width)
        flat_out = finish_layer(o_part, ml.reshape(n_batch, 2 * rows_q), x_own, mlp_norm, w_o, w_gate, w_up, w_down,
                                n_steps, heads, exp_scale)
        hid_out = flat_out.reshape(4 * n_chunks, n_steps, per_chunk, width).transpose(1, 0, 2, 3).reshape(n_steps, n_batch, width)
        return hid_out, k_out.reshape(k_cache.shape), v_out.reshape(v_cache.shape)

    return jax.shard_map(shard_body, mesh=mesh, in_specs=in_specs, out_specs=out_specs, check_vma=False)
```

```python
import functools
import math

import jax
import jax.numpy as jnp
from jax import lax
from jax.experimental import pallas as pl
from jax.experimental.pallas import tpu as pltpu
from jax.sharding import PartitionSpec as P

ROPE_BASE = 1000000.0
NORM_EPS = 1e-06
MASKED = -3e38
FLOOR = -1e38


def rms_scale(values, gain_vec):
    wide_vals = values.astype(jnp.float32)
    inv_rms = lax.rsqrt(jnp.mean(wide_vals * wide_vals, axis=-1, keepdims=True) + NORM_EPS)
    return wide_vals * inv_rms * gain_vec.astype(jnp.float32)


def rope_tables(tok_pos, head_dim):
    half_dim = head_dim // 2
    freqs = ROPE_BASE ** (-(jnp.arange(half_dim, dtype=jnp.float32) * (2.0 / head_dim)))
    angles = tok_pos.astype(jnp.float32)[:, None] * freqs[None, :]
    cos_tab = jnp.cos(angles)
    sin_tab = jnp.sin(angles)
    return jnp.concatenate([cos_tab, cos_tab], axis=-1), jnp.concatenate([-sin_tab, sin_tab], axis=-1)


def qkv_kernel(dims, x_ref, norm_ref, cos_ref, sin_ref, qg_ref, kg_ref, wq_hbm, wk_hbm, wv_hbm, q_ref, k_ref, v_ref,
               n_ref, y_ref, qf_ref, wbuf, sems):
    heads, kv_heads, hd, unit, n_buf = dims
    tokens = x_ref.shape[0]
    rows_blk = 64
    per = unit // hd
    n_q, n_kv = heads // per, kv_heads // per
    total = n_q + 2 * n_kv

    def fetch(hbm, col, slot):
        return pltpu.make_async_copy(hbm.at[:, pl.ds(pl.multiple_of(col * unit, unit), unit)], wbuf.at[slot], sems.at[slot])

    def start(g):
        slot = lax.rem(g, n_buf)

        @pl.when(g < n_q)
        def _():
            fetch(wq_hbm, g, slot).start()

        @pl.when((g >= n_q) & (g < n_q + n_kv))
        def _():
            fetch(wk_hbm, g - n_q, slot).start()

        @pl.when((g >= n_q + n_kv) & (g < total))
        def _():
            fetch(wv_hbm, g - n_q - n_kv, slot).start()

    for g in range(n_buf - 1):
        start(jnp.int32(g))

    def norm_rows(i, carry):
        rows = pl.ds(pl.multiple_of(i * rows_blk, rows_blk), rows_blk)
        wide = x_ref[rows, :].astype(jnp.float32)
        inv = lax.rsqrt(jnp.mean(wide * wide, axis=-1, keepdims=True) + NORM_EPS)
        n_ref[rows, :] = (wide * inv * norm_ref[...].astype(jnp.float32)).astype(n_ref.dtype)
        return carry

    lax.fori_loop(0, tokens // rows_blk, norm_rows, 0)

    def project(g):
        slot = lax.rem(g, n_buf)
        start(g + n_buf - 1)
        fetch(wq_hbm, 0, slot).wait()
        y_ref[...] = jnp.dot(n_ref[...], wbuf[slot], preferred_element_type=jnp.float32)

    def rotate(vec, gain_ref):
        inv = lax.rsqrt(jnp.mean(vec * vec, axis=-1, keepdims=True) + NORM_EPS)
        vec = vec * inv * gain_ref[...].astype(jnp.float32)
        return vec * cos_ref[...] + pltpu.roll(vec, hd // 2, 1) * sin_ref[...]

    def q_unit(g, carry):
        project(g)
        for h in range(per):
            qf_ref[pl.ds(g * per + h, tokens, stride=heads), :] = rotate(y_ref[:, h * hd:(h + 1) * hd], qg_ref)
        return carry

    lax.fori_loop(0, n_q, q_unit, 0)

    def k_unit(g, carry):
        project(n_q + g)
        for h in range(per):
            row = rotate(y_ref[:, h * hd:(h + 1) * hd], kg_ref).astype(jnp.bfloat16)
            k_ref[pl.ds(g * per + h, tokens, stride=kv_heads), :] = row.astype(jnp.float32)
        return carry

    lax.fori_loop(0, n_kv, k_unit, 0)

    def v_unit(g, carry):
        project(n_q + n_kv + g)
        for h in range(per):
            row = y_ref[:, h * hd:(h + 1) * hd].astype(jnp.bfloat16)
            v_ref[pl.ds(g * per + h, tokens, stride=kv_heads), :] = row.astype(jnp.float32)
        return carry

    lax.fori_loop(0, n_kv, v_unit, 0)

    def cast_rows(i, carry):
        rows = pl.ds(pl.multiple_of(i * 512, 512), 512)
        q_ref[rows, :] = qf_ref[rows, :].astype(q_ref.dtype)
        return carry

    lax.fori_loop(0, tokens * heads // 512, cast_rows, 0)


def project_qkv(x, norm, cos_tab, sin_tab, q_gain, k_gain, w_q, w_k, w_v):
    tokens, width = x.shape
    hd = q_gain.shape[0]
    heads, kv_heads = w_q.shape[1] // hd, w_k.shape[1] // hd
    unit, n_buf = 2 * hd, 4
    vmem = pl.BlockSpec(memory_space=pltpu.VMEM)
    hbm = pl.BlockSpec(memory_space=pl.ANY)
    cols = (heads + 2 * kv_heads) * hd
    return pl.pallas_call(
        functools.partial(qkv_kernel, (heads, kv_heads, hd, unit, n_buf)),
        in_specs=[vmem] * 6 + [hbm] * 3,
        out_specs=[vmem] * 3,
        out_shape=[jax.ShapeDtypeStruct((tokens * heads, hd), jnp.bfloat16),
                   jax.ShapeDtypeStruct((tokens * kv_heads, hd), jnp.float32),
                   jax.ShapeDtypeStruct((tokens * kv_heads, hd), jnp.float32)],
        scratch_shapes=[pltpu.VMEM((tokens, width), jnp.bfloat16),
                        pltpu.VMEM((tokens, unit), jnp.float32),
                        pltpu.VMEM((tokens * heads, hd), jnp.float32),
                        pltpu.VMEM((n_buf, width, unit), jnp.bfloat16),
                        pltpu.SemaphoreType.DMA((n_buf,))],
        compiler_params=pltpu.CompilerParams(vmem_limit_bytes=48 * 2**20),
        cost_estimate=pl.CostEstimate(flops=2 * tokens * width * cols, bytes_accessed=2 * width * cols, transcendentals=0),
        name="project_qkv",
    )(x, norm.reshape(1, width), cos_tab, sin_tab, q_gain.reshape(1, hd), k_gain.reshape(1, hd), w_q, w_k, w_v)


def attn_kernel(dims, order_ref, rel_ref, q_ref, kn_ref, vn_ref, k_ref, v_ref, ko_ref, vo_ref, o_ref, ml_ref):
    n_req, n_steps, heads, kv_heads, groups, rows_c, hd, exp_scale = dims
    rows_q = n_steps * heads
    new_rows = n_steps * kv_heads
    blk = order_ref[pl.program_id(0)]

    col = lax.broadcasted_iota(jnp.int32, (rows_q, rows_c), 1)
    row = lax.broadcasted_iota(jnp.int32, (rows_q, rows_c), 0)
    same_head = (col % kv_heads) == ((row % heads) // groups)
    lag = jnp.where(same_head, col // kv_heads - row // heads, jnp.int32(1 << 30))
    win_row = lax.broadcasted_iota(jnp.int32, (2 * new_rows, hd), 0)
    ml_lane = lax.broadcasted_iota(jnp.int32, (rows_q, 2 * rows_q), 1)
    ml_row = lax.broadcasted_iota(jnp.int32, (rows_q, 2 * rows_q), 0)
    pad = jnp.zeros((new_rows, hd), jnp.float32)

    for j in range(n_req):
        rel = rel_ref[blk * n_req + j]
        first = rel * kv_heads
        base = pl.multiple_of(jnp.clip((first >> 4) << 4, 0, rows_c - 2 * new_rows), 16)
        off = first - base
        inside = (win_row >= off) & (win_row < off + new_rows)
        for src, new, dst in ((k_ref, kn_ref, ko_ref), (v_ref, vn_ref, vo_ref)):
            dst[j] = src[j]
            fresh = [new[t, j * kv_heads:(j + 1) * kv_heads, :] for t in range(n_steps)]
            rolled = pltpu.roll(jnp.concatenate(fresh + [pad], axis=0), off & (2 * new_rows - 1), 0)
            window = src[j, pl.ds(base, 2 * new_rows), :].astype(jnp.float32)
            dst[j, pl.ds(base, 2 * new_rows), :] = jnp.where(inside, rolled, window).astype(dst.dtype)
        query = q_ref[:, j].reshape(rows_q, hd)
        scores = lax.dot_general(query, ko_ref[j], (((1,), (1,)), ((), ())), preferred_element_type=jnp.float32)
        scores = jnp.where(lag <= rel, scores, MASKED)
        top = jnp.maximum(jnp.max(scores, axis=1, keepdims=True), FLOOR)
        probs = jnp.exp2((scores - top) * exp_scale)
        total = jnp.sum(probs, axis=1, keepdims=True)
        o_ref[j] = lax.dot_general(probs.astype(jnp.bfloat16), vo_ref[j], (((1,), (0,)), ((), ())), preferred_element_type=jnp.float32)
        packed = jnp.where(ml_lane == ml_row, top, jnp.where(ml_lane == ml_row + rows_q, total, 0.0))
        ml_ref[j] = jnp.sum(packed, axis=0, keepdims=True)


def attention(order, rel, q, k_new, v_new, k_cache, v_cache, kv_heads, exp_scale, n_req=4):
    n_steps, n_batch, heads, hd = q.shape
    rows_c = k_cache.shape[1]
    rows_q = n_steps * heads
    dims = (n_req, n_steps, heads, kv_heads, heads // kv_heads, rows_c, hd, exp_scale)
    cache_blk = pl.BlockSpec((n_req, rows_c, hd), lambda i, order, rel: (order[i], 0, 0))
    new_blk = pl.BlockSpec((n_steps, n_req * kv_heads, hd), lambda i, order, rel: (0, order[i], 0))
    cache_shape = jax.ShapeDtypeStruct(k_cache.shape, k_cache.dtype)
    return pl.pallas_call(
        functools.partial(attn_kernel, dims),
        grid_spec=pltpu.PrefetchScalarGridSpec(
            num_scalar_prefetch=2,
            grid=(n_batch // n_req,),
            in_specs=[pl.BlockSpec((n_steps, n_req, heads, hd), lambda i, order, rel: (0, order[i], 0, 0)),
                      new_blk, new_blk, cache_blk, cache_blk],
            out_specs=[cache_blk, cache_blk,
                       pl.BlockSpec((n_req, rows_q, hd), lambda i, order, rel: (i, 0, 0)),
                       pl.BlockSpec((n_req, 1, 2 * rows_q), lambda i, order, rel: (i, 0, 0))],
        ),
        out_shape=[cache_shape, cache_shape,
                   jax.ShapeDtypeStruct((n_batch, rows_q, hd), jnp.float32),
                   jax.ShapeDtypeStruct((n_batch, 1, 2 * rows_q), jnp.float32)],
        compiler_params=pltpu.CompilerParams(dimension_semantics=("arbitrary",), vmem_limit_bytes=40 * 2**20),
        cost_estimate=pl.CostEstimate(flops=4 * n_batch * rows_q * rows_c * hd, bytes_accessed=8 * n_batch * rows_c * hd,
                                      transcendentals=n_batch * rows_q * rows_c),
        name="decode_attention",
    )(order, rel, q, k_new, v_new, k_cache, v_cache)


def tail_kernel(dims, o_ref, ml_ref, x_ref, gain_ref, wo_hbm, wg_hbm, wu_hbm, wd_hbm, out_ref,
                ring, near1, nml, far1, fml, wts, comb, attn, part_o, recv_o, res, mid, mid_out, mid_in, act,
                part_d, other_d, other_in, fin, across, near, diag,
                ring_sem, n1s, n1r, nms, nmr, f1s, f1r, fms, fmr, os_, or_, ms_, mr_, ps_, pr_, ds_, dr_, xs_, xr_, cs_, cr_, gs_, gr_):
    n_steps, heads, hd, n_chunks, exp_scale, n_slots = dims
    rows_q = n_steps * heads
    own = far1.shape[0]
    per = own // n_chunks
    tok = per * n_steps
    width = x_ref.shape[1]
    n_tok = x_ref.shape[0]
    hrows = n_tok // 2
    kt, nt = ring.shape[1], ring.shape[2]
    inner = act.shape[1]
    n_o, k_o = width // nt, heads * hd // kt
    n_up, k_up = inner // nt, width // kt
    n_dn, k_dn = width // nt, inner // kt
    first_mlp = n_o * k_o
    up_loads, dn_loads = 2 * k_up * n_up, k_dn * n_dn
    mlp_loads = up_loads + dn_loads
    n_loads = first_mlp + 2 * mlp_loads

    sp = lax.axis_index('sp')
    tp = lax.axis_index('tp')
    core = lax.rem(sp, 2)
    sp_core = sp + 1 - 2 * core
    sp_chip = lax.rem(sp + 2, 4)
    sp_diag = lax.rem(sp_core + 2, 4)
    to_core = {'sp': sp_core}
    to_chip = {'sp': sp_chip}
    to_tp = {'tp': 1 - tp}

    def send(src, dst, s_sem, r_sem, dev):
        return pltpu.make_async_remote_copy(src_ref=src, dst_ref=dst, send_sem=s_sem, recv_sem=r_sem, device_id=dev,
                                            device_id_type=pl.DeviceIdType.MESH)

    barrier = pltpu.get_barrier_semaphore()
    for dev in (to_core, to_chip, to_tp):
        pl.semaphore_signal(barrier, inc=1, device_id=dev, device_id_type=pl.DeviceIdType.MESH)
    pl.semaphore_wait(barrier, 3)

    near_ml = send(ml_ref.at[pl.ds(0, 2 * own)], nml, nms.at[0], nmr.at[0], to_core)
    near_ml.start()
    near_o = []
    for piece in (0, 1):
        for j in range(n_chunks):
            rows = pl.ds(piece * own + j * per, per)
            near_o.append(send(o_ref.at[rows], near1.at[rows], n1s.at[piece * n_chunks + j], n1r.at[piece * n_chunks + j], to_core))
    for copy in near_o:
        copy.start()

    def load(src, row, col, slot):
        return pltpu.make_async_copy(src.at[pl.ds(pl.multiple_of(row, kt), kt), pl.ds(pl.multiple_of(col, nt), nt)],
                                     ring.at[slot], ring_sem.at[slot])

    def start(idx):
        slot = lax.rem(idx, n_slots)

        @pl.when(idx < first_mlp)
        def _():
            load(wo_hbm, lax.rem(idx, k_o) * kt, (idx // k_o) * nt, slot).start()

        loc = lax.rem(idx - first_mlp + mlp_loads, mlp_loads)
        in_mlp = (idx >= first_mlp) & (idx < n_loads)
        sub = lax.rem(loc, 2 * k_up)
        up_col = core * inner + (loc // (2 * k_up)) * nt

        @pl.when(in_mlp & (loc < up_loads) & (sub < k_up))
        def _():
            load(wg_hbm, sub * kt, up_col, slot).start()

        @pl.when(in_mlp & (loc < up_loads) & (sub >= k_up))
        def _():
            load(wu_hbm, (sub - k_up) * kt, up_col, slot).start()

        dn = loc - up_loads

        @pl.when(in_mlp & (loc >= up_loads))
        def _():
            load(wd_hbm, core * inner + lax.rem(dn, k_dn) * kt, (dn // k_dn) * nt, slot).start()

    def arrived(idx):
        slot = lax.rem(idx, n_slots)
        load(wo_hbm, 0, 0, slot).wait()
        return slot

    def start_many(lo, hi):
        def one(i, carry):
            start(i)
            return carry
        lax.fori_loop(lo, hi, one, 0)

    start_many(0, n_slots)

    diag_mask = lax.broadcasted_iota(jnp.int32, (rows_q, 2 * rows_q), 0) == lax.broadcasted_iota(jnp.int32, (rows_q, 2 * rows_q), 1)
    left = lax.broadcasted_iota(jnp.int32, (per, 2 * rows_q), 1) < rows_q

    def column(row):
        return jnp.sum(jnp.where(diag_mask, row, 0.0), axis=1, keepdims=True)

    def weights(stat_a, stat_b):
        top = jnp.maximum(stat_a, stat_b)
        wt_a = jnp.exp2((stat_a - top) * exp_scale)
        wt_b = jnp.exp2((stat_b - top) * exp_scale)
        total = pltpu.roll(wt_a, rows_q, 1) * stat_a + pltpu.roll(wt_b, rows_q, 1) * stat_b
        return wt_a, wt_b, jnp.where(left, top, total)

    def merge_near(piece, j):
        base = piece * own + j * per
        near_o[piece * n_chunks + j].wait_recv()
        wt_a, wt_b, stat = weights(nml[base:base + per, :], ml_ref[2 * own + base:2 * own + base + per, :])
        wts[0] = wt_a
        wts[1] = wt_b
        nml[base:base + per, :] = stat

        def one(i, carry):
            near1[base + i] = column(wts[0, pl.ds(i, 1), :]) * near1[base + i] + column(wts[1, pl.ds(i, 1), :]) * o_ref[2 * own + base + i]
            return carry
        lax.fori_loop(0, per, one, 0)

    near_ml.wait_recv()
    far_o, far_ml = [], []
    for j in range(n_chunks):
        rows = pl.ds(j * per, per)
        merge_near(0, j)
        far_ml.append(send(nml.at[rows], fml.at[rows], fms.at[j], fmr.at[j], to_chip))
        far_o.append(send(near1.at[rows], far1.at[rows], f1s.at[j], f1r.at[j], to_chip))
        far_ml[j].start()
        far_o[j].start()
    for j in range(n_chunks):
        merge_near(1, j)

    tp_o = []
    for j in range(n_chunks):
        base = j * per
        far_ml[j].wait_recv()
        far_o[j].wait_recv()
        wt_a, wt_b, stat = weights(nml[own + base:own + base + per, :], fml[base:base + per, :])
        inv = pltpu.roll(1.0 / stat, rows_q, 1)
        wts[0] = wt_a * inv
        wts[1] = wt_b * inv

        def one(i, carry, base=base):
            rows = pl.ds(pl.multiple_of(i * rows_q, rows_q), rows_q)
            comb[rows, :] = column(wts[0, pl.ds(i, 1), :]) * near1[own + base + i] + column(wts[1, pl.ds(i, 1), :]) * far1[base + i]
            return carry
        lax.fori_loop(0, per, one, 0)
        for step in range(n_steps):
            for h in range(heads):
                attn[step * per:(step + 1) * per, h * hd:(h + 1) * hd] = comb[pl.ds(step * heads + h, per, stride=rows_q), :]
        attn_in = attn[...].astype(jnp.bfloat16)

        def o_tile(n, carry, j=j, attn_in=attn_in):
            acc = None
            for k in range(k_o):
                if j == 0:
                    arrived(n * k_o + k)
                prod = jnp.dot(attn_in[:, k * kt:(k + 1) * kt], ring[n * k_o + k], preferred_element_type=jnp.float32)
                acc = prod if acc is None else acc + prod
            part_o[j, :, pl.ds(pl.multiple_of(n * nt, nt), nt)] = acc
            return carry
        lax.fori_loop(0, n_o, o_tile, 0)
        tp_o.append(send(part_o.at[j], recv_o.at[j], os_.at[j], or_.at[j], to_tp))
        tp_o[j].start()
    start_many(n_slots, n_slots + first_mlp)

    mid_x = [send(mid_out.at[j], mid_in.at[j], ms_.at[j], mr_.at[j], to_core) for j in range(n_chunks)]

    def pair_d(h, t):
        return send(other_d.at[h, t], other_in.at[h, t], ps_.at[h, t], pr_.at[h, t], to_core)

    def tp_d(h, t):
        return send(part_d.at[h, t], fin.at[h, t], ds_.at[h, t], dr_.at[h, t], to_tp)

    def chip_d(h, t):
        return send(fin.at[h, t], across.at[h, t], xs_.at[h, t], xr_.at[h, t], to_chip)

    def core_d(h, t):
        return send(fin.at[h, t], near.at[h, t], cs_.at[h, t], cr_.at[h, t], to_core)

    def diag_d(h, t):
        return send(across.at[h, t], diag.at[h, t], gs_.at[h, t], gr_.at[h, t], to_core)

    def cols(t):
        return pl.ds(t * nt if isinstance(t, int) else pl.multiple_of(t * nt, nt), nt)

    def emit(who, h, t, value):
        rows = pl.ds(pl.multiple_of(who * n_tok + h * hrows, hrows), hrows)
        out_ref[rows, cols(t)] = value.astype(out_ref.dtype)

    half = 16

    def residual(j):
        tp_o[j].wait_recv()
        h, low = j // 2, (j % 2) * tok

        def norm_rows(i, carry):
            sub = pl.ds(pl.multiple_of(i * half, half), half)
            rows = pl.ds(pl.multiple_of(j * tok + i * half, half), half)
            summed = x_ref[rows, :].astype(jnp.float32) + (part_o[j, sub, :] + recv_o[j, sub, :])
            resid = summed.astype(jnp.bfloat16)
            res[rows, :] = resid
            wide = resid.astype(jnp.float32)
            inv = lax.rsqrt(jnp.mean(wide * wide, axis=-1, keepdims=True) + NORM_EPS)
            scaled = wide * inv * gain_ref[...].astype(jnp.float32)
            mid_out[j, sub, :] = scaled
            mid[h, pl.ds(pl.multiple_of(low + i * half, half), half), :] = scaled.astype(jnp.bfloat16)
            return carry
        lax.fori_loop(0, tok // half, norm_rows, 0)
        mid_x[j].start()

    def partner(j):
        mid_x[j].wait_recv()
        h, low = j // 2, hrows + (j % 2) * tok

        def copy_rows(i, carry):
            sub = pl.ds(pl.multiple_of(i * half, half), half)
            mid[h, pl.ds(pl.multiple_of(low + i * half, half), half), :] = mid_in[j, sub, :].astype(jnp.bfloat16)
            return carry
        lax.fori_loop(0, tok // half, copy_rows, 0)

    def up_tile(h, t):
        idx = first_mlp + h * mlp_loads + 2 * k_up * t
        total = []
        for side in (0, 1):
            acc = None
            for k in range(k_up):
                slot = arrived(idx + side * k_up + k)
                prod = jnp.dot(mid[h, :, k * kt:(k + 1) * kt], ring[slot], preferred_element_type=jnp.float32)
                acc = prod if acc is None else acc + prod
            total.append(acc)
        gate, up = total
        act[:, cols(t)] = (jax.nn.silu(gate) * up).astype(jnp.bfloat16)
        for k in range(2 * k_up):
            start(idx + k + n_slots)

    def down(h, t):
        idx = first_mlp + h * mlp_loads + up_loads + k_dn * t
        acc = None
        for k in range(k_dn):
            slot = arrived(idx + k)
            prod = jnp.dot(act[:, k * kt:(k + 1) * kt], ring[slot], preferred_element_type=jnp.float32)
            acc = prod if acc is None else acc + prod
        part_d[h, t] = acc[:hrows]
        other_d[h, t] = acc[hrows:]
        pair_d(h, t).start()
        for k in range(k_dn):
            start(idx + k + n_slots)

    def reduce(h, t):
        pair_d(h, t).wait_recv()
        part_d[h, t] = part_d[h, t] + other_in[h, t]
        tp_d(h, t).start()

    def finish(h, t):
        tp_d(h, t).wait_recv()
        fin[h, t] = res[h * hrows:(h + 1) * hrows, cols(t)].astype(jnp.float32) + (part_d[h, t] + fin[h, t])
        chip_d(h, t).start()
        core_d(h, t).start()
        emit(sp, h, t, fin[h, t])

    def forward(h, t):
        chip_d(h, t).wait_recv()
        diag_d(h, t).start()
        emit(sp_chip, h, t, across[h, t])
        core_d(h, t).wait_recv()
        emit(sp_core, h, t, near[h, t])

    def collect(h, t):
        diag_d(h, t).wait_recv()
        emit(sp_diag, h, t, diag[h, t])

    def loop(lo, hi, fn):
        def one(t, carry):
            fn(t)
            return carry
        lax.fori_loop(lo, hi, one, 0)

    def down_then_reduce(h):
        def one(t):
            down(h, t)
            reduce(h, t - 1)
        return one

    for j in (0, 1):
        residual(j)
    for j in (0, 1):
        partner(j)
    loop(0, n_up, lambda t: up_tile(0, t))
    down(0, 0)
    loop(1, n_dn, down_then_reduce(0))
    reduce(0, n_dn - 1)

    for j in (2, 3):
        residual(j)
    for j in (2, 3):
        partner(j)
    up_tile(1, 0)

    def up_then_finish(t):
        up_tile(1, t)
        finish(0, t - 1)

    loop(1, n_up, up_then_finish)
    down(1, 0)
    finish(0, n_up - 1)

    def down_more(t):
        down(1, t)
        reduce(1, t - 1)

    loop(1, 3, down_more)
    finish(0, n_up)
    loop(3, 5, down_more)
    finish(0, n_up + 1)
    loop(5, n_dn, down_more)
    reduce(1, n_dn - 1)
    loop(0, n_dn // 2, lambda t: forward(0, t))

    def wind_a(t):
        finish(1, t)
        forward(0, t + n_dn // 2)

    loop(0, n_dn // 2, wind_a)

    def wind_b(t):
        finish(1, t)
        forward(1, t - n_dn // 2)
        collect(0, t - n_dn // 2)

    loop(n_dn // 2, n_dn, wind_b)

    def wind_c(t):
        collect(0, t)
        forward(1, t)
        collect(1, t - n_dn // 2)

    loop(n_dn // 2, n_dn, wind_c)
    loop(n_dn // 2, n_dn, lambda t: collect(1, t))

    for copy in near_o + [near_ml] + far_o + far_ml + tp_o + mid_x:
        copy.wait_send()
    for h in (0, 1):
        for build in (pair_d, tp_d, chip_d, core_d, diag_d):
            loop(0, n_dn, lambda t, h=h, build=build: build(h, t).wait_send())


def finish_layer(o_part, ml, x_own, norm, w_o, w_gate, w_up, w_down, n_steps, heads, exp_scale):
    n_batch, rows_q, hd = o_part.shape
    tokens, width = x_own.shape
    own = tokens // n_steps
    inner = w_gate.shape[1] // 2
    n_chunks, n_slots, kt, nt = 4, 20, 1024, 512
    per = own // n_chunks
    n_dn = width // nt
    vmem = pl.BlockSpec(memory_space=pltpu.VMEM)
    hbm = pl.BlockSpec(memory_space=pl.ANY)
    f32, bf16 = jnp.float32, jnp.bfloat16
    tiles = pltpu.VMEM((2, n_dn, tokens // 2, nt), f32)
    chunk = pltpu.VMEM((n_chunks, per * n_steps, width), f32)
    dma = pltpu.SemaphoreType.DMA
    return pl.pallas_call(
        functools.partial(tail_kernel, (n_steps, heads, hd, n_chunks, exp_scale, n_slots)),
        in_specs=[vmem] * 4 + [hbm] * 4,
        out_specs=vmem,
        out_shape=jax.ShapeDtypeStruct((4 * tokens, width), bf16),
        scratch_shapes=[pltpu.VMEM((n_slots, kt, nt), bf16),
                        pltpu.VMEM((2 * own, rows_q, hd), f32), pltpu.VMEM((2 * own, 2 * rows_q), f32),
                        pltpu.VMEM((own, rows_q, hd), f32), pltpu.VMEM((own, 2 * rows_q), f32),
                        pltpu.VMEM((2, per, 2 * rows_q), f32), pltpu.VMEM((per * rows_q, hd), f32),
                        pltpu.VMEM((per * n_steps, heads * hd), f32),
                        chunk, chunk,
                        pltpu.VMEM((tokens, width), bf16), pltpu.VMEM((2, tokens, width), bf16), chunk, chunk,
                        pltpu.VMEM((tokens, inner), bf16),
                        tiles, tiles, tiles, tiles, tiles, tiles, tiles,
                        dma((n_slots,)), dma((2 * n_chunks,)), dma((2 * n_chunks,)), dma((1,)), dma((1,)),
                        dma((n_chunks,)), dma((n_chunks,)), dma((n_chunks,)), dma((n_chunks,)), dma((n_chunks,)), dma((n_chunks,)),
                        dma((n_chunks,)), dma((n_chunks,))] + [dma((2, n_dn))] * 10,
        compiler_params=pltpu.CompilerParams(collective_id=0, has_side_effects=True, vmem_limit_bytes=63 * 2**20),
        name="finish_layer",
    )(o_part, ml, x_own, norm.reshape(1, width), w_o, w_gate, w_up, w_down)


def solution(mesh):
    cache_spec = P('dp', 'sp', 'tp', None)
    col_spec = P(None, 'tp')
    row_spec = P('tp', None)
    in_specs = (P(None, 'dp', None), P('dp'), cache_spec, cache_spec, col_spec, col_spec, col_spec, row_spec,
                col_spec, col_spec, row_spec, P(), P(), P(), P())
    out_specs = (P(None, 'dp', None), cache_spec, cache_spec)

    def shard_body(hidden, start_pos, k_cache, v_cache, w_q, w_k, w_v, w_o, w_gate, w_up, w_down, attn_norm, mlp_norm, q_gain, k_gain):
        n_steps, n_batch, width = hidden.shape
        seq_blk, kv_heads, hd = k_cache.shape[1], k_cache.shape[2], k_cache.shape[3]
        heads = w_q.shape[1] // hd
        rows_q = n_steps * heads
        exp_scale = hd ** -0.5 * math.log2(math.e)
        sp = lax.axis_index('sp')
        core, chip = sp % 2, sp // 2
        own = n_batch // 4

        tok_pos = (start_pos[None, :] + jnp.arange(n_steps, dtype=jnp.int32)[:, None]).reshape(-1)
        cos_tab, sin_tab = rope_tables(tok_pos, hd)
        q_rows, k_rows, v_rows = project_qkv(hidden.reshape(n_steps * n_batch, width), attn_norm, cos_tab, sin_tab,
                                             q_gain, k_gain, w_q, w_k, w_v)
        q_rot = q_rows.reshape(n_steps, n_batch, heads, hd)
        k_rows = k_rows.reshape(n_steps, n_batch * kv_heads, hd)
        v_rows = v_rows.reshape(n_steps, n_batch * kv_heads, hd)

        n_req = 4
        per = own // n_req
        part = jnp.stack([(1 - chip) * 2 + (1 - core), chip * 2 + (1 - core), (1 - chip) * 2 + core, chip * 2 + core])
        order = (part[:, None] * per + jnp.arange(per)[None, :]).reshape(-1).astype(jnp.int32)
        rel = start_pos - sp * seq_blk
        flat = (n_batch, seq_blk * kv_heads, hd)
        k_out, v_out, o_part, ml = attention(order, rel, q_rot, k_rows, v_rows, k_cache.reshape(flat), v_cache.reshape(flat),
                                             kv_heads, exp_scale, n_req)

        n_chunks = 4
        per_chunk = own // n_chunks
        x_own = lax.dynamic_slice_in_dim(hidden, sp * own, own, axis=1).reshape(n_steps, n_chunks, per_chunk, width)
        x_own = x_own.transpose(1, 0, 2, 3).reshape(n_steps * own, width)
        flat_out = finish_layer(o_part, ml.reshape(n_batch, 2 * rows_q), x_own, mlp_norm, w_o, w_gate, w_up, w_down,
                                n_steps, heads, exp_scale)
        hid_out = flat_out.reshape(4 * n_chunks, n_steps, per_chunk, width).transpose(1, 0, 2, 3).reshape(n_steps, n_batch, width)
        return hid_out, k_out.reshape(k_cache.shape), v_out.reshape(v_cache.shape)

    return jax.shard_map(shard_body, mesh=mesh, in_specs=in_specs, out_specs=out_specs, check_vma=False)
```

```python
import functools
import math

import jax
import jax.numpy as jnp
from jax import lax
from jax.experimental import pallas as pl
from jax.experimental.pallas import tpu as pltpu
from jax.sharding import PartitionSpec as P

ROPE_BASE = 1000000.0
NORM_EPS = 1e-06
MASKED = -3e38
FLOOR = -1e38


def rms_scale(values, gain_vec):
    wide_vals = values.astype(jnp.float32)
    inv_rms = lax.rsqrt(jnp.mean(wide_vals * wide_vals, axis=-1, keepdims=True) + NORM_EPS)
    return wide_vals * inv_rms * gain_vec.astype(jnp.float32)


def rope_tables(tok_pos, head_dim):
    half_dim = head_dim // 2
    freqs = ROPE_BASE ** (-(jnp.arange(half_dim, dtype=jnp.float32) * (2.0 / head_dim)))
    angles = tok_pos.astype(jnp.float32)[:, None] * freqs[None, :]
    cos_tab = jnp.cos(angles)
    sin_tab = jnp.sin(angles)
    return jnp.concatenate([cos_tab, cos_tab], axis=-1), jnp.concatenate([-sin_tab, sin_tab], axis=-1)


def qkv_kernel(dims, x_ref, norm_ref, cos_ref, sin_ref, qg_ref, kg_ref, wq_hbm, wk_hbm, wv_hbm, q_ref, k_ref, v_ref,
               n_ref, ya_ref, yb_ref, qf_ref, wbuf, sems):
    heads, kv_heads, hd, unit, n_buf = dims
    tokens = x_ref.shape[0]
    rows_blk = 64
    per = unit // hd
    n_q, n_kv = heads // per, kv_heads // per
    total = n_q + 2 * n_kv

    units = [(wk_hbm, g, k_ref, kg_ref) for g in range(n_kv)] + [(wv_hbm, g, v_ref, None) for g in range(n_kv)]
    units += [(wq_hbm, g, qf_ref, qg_ref) for g in range(n_q)]

    def fetch(g):
        hbm, col, _, _ = units[g]
        slot = g % n_buf
        return pltpu.make_async_copy(hbm.at[:, pl.ds(col * unit, unit)], wbuf.at[slot], sems.at[slot])

    for g in range(n_buf - 1):
        fetch(g).start()

    def norm_rows(i, carry):
        rows = pl.ds(pl.multiple_of(i * rows_blk, rows_blk), rows_blk)
        wide = x_ref[rows, :].astype(jnp.float32)
        inv = lax.rsqrt(jnp.mean(wide * wide, axis=-1, keepdims=True) + NORM_EPS)
        n_ref[rows, :] = (wide * inv * norm_ref[...].astype(jnp.float32)).astype(n_ref.dtype)
        return carry

    lax.fori_loop(0, tokens // rows_blk, norm_rows, 0)

    def rotate(vec, rows, gain_ref):
        inv = lax.rsqrt(jnp.mean(vec * vec, axis=-1, keepdims=True) + NORM_EPS)
        vec = vec * inv * gain_ref[...].astype(jnp.float32)
        return vec * cos_ref[rows, :] + pltpu.roll(vec, hd // 2, 1) * sin_ref[rows, :]

    def store(g):
        _, col, dst, gain_ref = units[g]
        y_ref = (ya_ref, yb_ref)[g % 2]
        n_heads = heads if dst is qf_ref else kv_heads
        step = 64
        for low in range(0, tokens, step):
            for h in range(per):
                vec = y_ref[low:low + step, h * hd:(h + 1) * hd]
                if gain_ref is not None:
                    vec = rotate(vec, slice(low, low + step), gain_ref)
                if dst is not qf_ref:
                    vec = vec.astype(jnp.bfloat16).astype(jnp.float32)
                dst[pl.ds(low * n_heads + col * per + h, step, stride=n_heads), :] = vec

    for g in range(total):
        fetch(g).wait()
        for low in range(0, tokens, tokens // 2):
            rows = slice(low, low + tokens // 2)
            (ya_ref, yb_ref)[g % 2][rows, :] = jnp.dot(n_ref[rows, :], wbuf[g % n_buf], preferred_element_type=jnp.float32)
        if g > 0:
            store(g - 1)
        if g + n_buf - 1 < total:
            fetch(g + n_buf - 1).start()
    store(total - 1)

    def cast_rows(i, carry):
        rows = pl.ds(pl.multiple_of(i * 512, 512), 512)
        q_ref[rows, :] = qf_ref[rows, :].astype(q_ref.dtype)
        return carry

    lax.fori_loop(0, tokens * heads // 512, cast_rows, 0)


def project_qkv(x, norm, cos_tab, sin_tab, q_gain, k_gain, w_q, w_k, w_v):
    tokens, width = x.shape
    hd = q_gain.shape[0]
    heads, kv_heads = w_q.shape[1] // hd, w_k.shape[1] // hd
    unit, n_buf = 2 * hd, 4
    vmem = pl.BlockSpec(memory_space=pltpu.VMEM)
    hbm = pl.BlockSpec(memory_space=pl.ANY)
    cols = (heads + 2 * kv_heads) * hd
    return pl.pallas_call(
        functools.partial(qkv_kernel, (heads, kv_heads, hd, unit, n_buf)),
        in_specs=[vmem] * 6 + [hbm] * 3,
        out_specs=[vmem] * 3,
        out_shape=[jax.ShapeDtypeStruct((tokens * heads, hd), jnp.bfloat16),
                   jax.ShapeDtypeStruct((tokens * kv_heads, hd), jnp.float32),
                   jax.ShapeDtypeStruct((tokens * kv_heads, hd), jnp.float32)],
        scratch_shapes=[pltpu.VMEM((tokens, width), jnp.bfloat16),
                        pltpu.VMEM((tokens, unit), jnp.float32),
                        pltpu.VMEM((tokens, unit), jnp.float32),
                        pltpu.VMEM((tokens * heads, hd), jnp.float32),
                        pltpu.VMEM((n_buf, width, unit), jnp.bfloat16),
                        pltpu.SemaphoreType.DMA((n_buf,))],
        compiler_params=pltpu.CompilerParams(vmem_limit_bytes=48 * 2**20),
        cost_estimate=pl.CostEstimate(flops=2 * tokens * width * cols, bytes_accessed=2 * width * cols, transcendentals=0),
        name="project_qkv",
    )(x, norm.reshape(1, width), cos_tab, sin_tab, q_gain.reshape(1, hd), k_gain.reshape(1, hd), w_q, w_k, w_v)


def attn_kernel(dims, order_ref, rel_ref, q_ref, kn_ref, vn_ref, k_ref, v_ref, ko_ref, vo_ref, o_ref, ml_ref,
                lag_ref, sa_ref, sb_ref, pa_ref, pb_ref):
    n_req, n_steps, heads, kv_heads, groups, rows_c, hd, exp_scale = dims
    rows_q = n_steps * heads
    new_rows = n_steps * kv_heads
    step_rows = 16
    blk = order_ref[pl.program_id(0)]

    @pl.when(pl.program_id(0) == 0)
    def _():
        col = lax.broadcasted_iota(jnp.int32, (rows_q, rows_c), 1)
        row = lax.broadcasted_iota(jnp.int32, (rows_q, rows_c), 0)
        same_head = (col % kv_heads) == ((row % heads) // groups)
        lag_ref[...] = jnp.where(same_head, col // kv_heads - row // heads, jnp.int32(1 << 30))

    win_row = lax.broadcasted_iota(jnp.int32, (2 * new_rows, hd), 0)
    ml_lane = lax.broadcasted_iota(jnp.int32, (step_rows, 2 * rows_q), 1)
    ml_row = lax.broadcasted_iota(jnp.int32, (step_rows, 2 * rows_q), 0)
    pad = jnp.zeros((new_rows, hd), jnp.float32)
    rels = [rel_ref[blk * n_req + j] for j in range(n_req)]

    def insert(j):
        first = rels[j] * kv_heads
        base = pl.multiple_of(jnp.clip((first >> 4) << 4, 0, rows_c - 2 * new_rows), 16)
        off = first - base
        inside = (win_row >= off) & (win_row < off + new_rows)
        for src, new, dst in ((k_ref, kn_ref, ko_ref), (v_ref, vn_ref, vo_ref)):
            dst[j] = src[j]
            fresh = [new[t, j * kv_heads:(j + 1) * kv_heads, :] for t in range(n_steps)]
            rolled = pltpu.roll(jnp.concatenate(fresh + [pad], axis=0), off & (2 * new_rows - 1), 0)
            window = src[j, pl.ds(base, 2 * new_rows), :].astype(jnp.float32)
            dst[j, pl.ds(base, 2 * new_rows), :] = jnp.where(inside, rolled, window).astype(dst.dtype)

    def score(j):
        query = q_ref[:, j].reshape(rows_q, hd)
        (sa_ref, sb_ref)[j % 2][...] = lax.dot_general(query, ko_ref[j], (((1,), (1,)), ((), ())),
                                                       preferred_element_type=jnp.float32)

    def attend(j):
        s_ref, p_ref = ((sa_ref, pa_ref), (sb_ref, pb_ref))[j % 2]
        stats = jnp.zeros((1, 2 * rows_q), jnp.float32)
        for low in range(0, rows_q, step_rows):
            rows = slice(low, low + step_rows)
            scores = jnp.where(lag_ref[rows, :] <= rels[j], s_ref[rows, :], MASKED)
            top = jnp.maximum(jnp.max(scores, axis=1, keepdims=True), FLOOR)
            probs = jnp.exp2((scores - top) * exp_scale)
            total = jnp.sum(probs, axis=1, keepdims=True)
            p_ref[rows, :] = probs.astype(jnp.bfloat16)
            packed = jnp.where(ml_lane == ml_row + low, top, jnp.where(ml_lane == ml_row + (low + rows_q), total, 0.0))
            stats = stats + jnp.sum(packed, axis=0, keepdims=True)
        ml_ref[j] = stats
        o_ref[j] = lax.dot_general(p_ref[...], vo_ref[j], (((1,), (0,)), ((), ())), preferred_element_type=jnp.float32)

    for j in range(n_req):
        insert(j)
    score(0)
    for j in range(n_req):
        if j + 1 < n_req:
            score(j + 1)
        attend(j)


def attention(order, rel, q, k_new, v_new, k_cache, v_cache, kv_heads, exp_scale, n_req=4):
    n_steps, n_batch, heads, hd = q.shape
    rows_c = k_cache.shape[1]
    rows_q = n_steps * heads
    dims = (n_req, n_steps, heads, kv_heads, heads // kv_heads, rows_c, hd, exp_scale)
    cache_blk = pl.BlockSpec((n_req, rows_c, hd), lambda i, order, rel: (order[i], 0, 0))
    new_blk = pl.BlockSpec((n_steps, n_req * kv_heads, hd), lambda i, order, rel: (0, order[i], 0))
    cache_shape = jax.ShapeDtypeStruct(k_cache.shape, k_cache.dtype)
    return pl.pallas_call(
        functools.partial(attn_kernel, dims),
        grid_spec=pltpu.PrefetchScalarGridSpec(
            num_scalar_prefetch=2,
            grid=(n_batch // n_req,),
            in_specs=[pl.BlockSpec((n_steps, n_req, heads, hd), lambda i, order, rel: (0, order[i], 0, 0)),
                      new_blk, new_blk, cache_blk, cache_blk],
            out_specs=[cache_blk, cache_blk,
                       pl.BlockSpec((n_req, rows_q, hd), lambda i, order, rel: (i, 0, 0)),
                       pl.BlockSpec((n_req, 1, 2 * rows_q), lambda i, order, rel: (i, 0, 0))],
            scratch_shapes=[pltpu.VMEM((rows_q, rows_c), jnp.int32)] + [pltpu.VMEM((rows_q, rows_c), jnp.float32)] * 2
                           + [pltpu.VMEM((rows_q, rows_c), jnp.bfloat16)] * 2,
        ),
        out_shape=[cache_shape, cache_shape,
                   jax.ShapeDtypeStruct((n_batch, rows_q, hd), jnp.float32),
                   jax.ShapeDtypeStruct((n_batch, 1, 2 * rows_q), jnp.float32)],
        compiler_params=pltpu.CompilerParams(dimension_semantics=("arbitrary",), vmem_limit_bytes=40 * 2**20),
        cost_estimate=pl.CostEstimate(flops=4 * n_batch * rows_q * rows_c * hd, bytes_accessed=8 * n_batch * rows_c * hd,
                                      transcendentals=n_batch * rows_q * rows_c),
        name="decode_attention",
    )(order, rel, q, k_new, v_new, k_cache, v_cache)


def tail_kernel(dims, o_ref, ml_ref, x_ref, gain_ref, wo_hbm, wg_hbm, wu_hbm, wd_hbm, out_ref,
                ring, near1, nml, far1, fml, comb, attn, part_o, recv_o, res, mid, mid_out, mid_in, act,
                part_d, other_d, other_in, fin, across, near, diag,
                ring_sem, n1s, n1r, nms, nmr, f1s, f1r, fms, fmr, os_, or_, ms_, mr_, ps_, pr_, ds_, dr_, xs_, xr_, cs_, cr_, gs_, gr_):
    n_steps, heads, hd, n_chunks, exp_scale, n_slots = dims
    rows_q = n_steps * heads
    own = far1.shape[0]
    per = own // n_chunks
    tok = per * n_steps
    width = x_ref.shape[1]
    n_tok = x_ref.shape[0]
    hrows = n_tok // 2
    kt, nt = ring.shape[1], ring.shape[2]
    inner = act.shape[1]
    n_o, k_o = width // nt, heads * hd // kt
    n_up, k_up = inner // nt, width // kt
    n_dn, k_dn = width // nt, inner // kt
    first_mlp = n_o * k_o
    up_loads, dn_loads = 2 * k_up * n_up, k_dn * n_dn
    mlp_loads = up_loads + dn_loads
    n_loads = first_mlp + 2 * mlp_loads

    sp = lax.axis_index('sp')
    tp = lax.axis_index('tp')
    core = lax.rem(sp, 2)
    sp_core = sp + 1 - 2 * core
    sp_chip = lax.rem(sp + 2, 4)
    sp_diag = lax.rem(sp_core + 2, 4)
    to_core = {'sp': sp_core}
    to_chip = {'sp': sp_chip}
    to_tp = {'tp': 1 - tp}

    def send(src, dst, s_sem, r_sem, dev):
        return pltpu.make_async_remote_copy(src_ref=src, dst_ref=dst, send_sem=s_sem, recv_sem=r_sem, device_id=dev,
                                            device_id_type=pl.DeviceIdType.MESH)

    barrier = pltpu.get_barrier_semaphore()
    for dev in (to_core, to_chip, to_tp):
        pl.semaphore_signal(barrier, inc=1, device_id=dev, device_id_type=pl.DeviceIdType.MESH)
    pl.semaphore_wait(barrier, 3)

    near_ml = send(ml_ref.at[pl.ds(0, 2 * own)], nml, nms.at[0], nmr.at[0], to_core)
    near_ml.start()
    near_o = []
    for piece in (0, 1):
        for j in range(n_chunks):
            rows = pl.ds(piece * own + j * per, per)
            near_o.append(send(o_ref.at[rows], near1.at[rows], n1s.at[piece * n_chunks + j], n1r.at[piece * n_chunks + j], to_core))
    for copy in near_o:
        copy.start()

    def load(src, row, col, slot):
        return pltpu.make_async_copy(src.at[pl.ds(pl.multiple_of(row, kt), kt), pl.ds(pl.multiple_of(col, nt), nt)],
                                     ring.at[slot], ring_sem.at[slot])

    def start(idx):
        slot = lax.rem(idx, n_slots)

        @pl.when(idx < first_mlp)
        def _():
            load(wo_hbm, lax.rem(idx, k_o) * kt, (idx // k_o) * nt, slot).start()

        loc = lax.rem(idx - first_mlp + mlp_loads, mlp_loads)
        in_mlp = (idx >= first_mlp) & (idx < n_loads)
        sub = lax.rem(loc, 2 * k_up)
        up_col = core * inner + (loc // (2 * k_up)) * nt

        @pl.when(in_mlp & (loc < up_loads) & (sub < k_up))
        def _():
            load(wg_hbm, sub * kt, up_col, slot).start()

        @pl.when(in_mlp & (loc < up_loads) & (sub >= k_up))
        def _():
            load(wu_hbm, (sub - k_up) * kt, up_col, slot).start()

        dn = loc - up_loads

        @pl.when(in_mlp & (loc >= up_loads))
        def _():
            load(wd_hbm, core * inner + lax.rem(dn, k_dn) * kt, (dn // k_dn) * nt, slot).start()

    def arrived(idx):
        slot = lax.rem(idx, n_slots)
        load(wo_hbm, 0, 0, slot).wait()
        return slot

    def start_many(lo, hi):
        def one(i, carry):
            start(i)
            return carry
        lax.fori_loop(lo, hi, one, 0)

    start_many(0, n_slots)

    diag_mask = lax.broadcasted_iota(jnp.int32, (rows_q, 2 * rows_q), 0) == lax.broadcasted_iota(jnp.int32, (rows_q, 2 * rows_q), 1)
    left = lax.broadcasted_iota(jnp.int32, (per, 2 * rows_q), 1) < rows_q

    def column(row):
        return jnp.sum(jnp.where(diag_mask, row, 0.0), axis=1, keepdims=True)

    def weights(stat_a, stat_b):
        top = jnp.maximum(stat_a, stat_b)
        wt_a = jnp.exp2((stat_a - top) * exp_scale)
        wt_b = jnp.exp2((stat_b - top) * exp_scale)
        total = pltpu.roll(wt_a, rows_q, 1) * stat_a + pltpu.roll(wt_b, rows_q, 1) * stat_b
        return wt_a, wt_b, jnp.where(left, top, total)

    def merge_near(piece, j):
        base = piece * own + j * per
        near_o[piece * n_chunks + j].wait_recv()
        wt_a, wt_b, stat = weights(nml[base:base + per, :], ml_ref[2 * own + base:2 * own + base + per, :])
        nml[base:base + per, :] = stat
        for i in range(per):
            near1[base + i] = column(wt_a[i:i + 1]) * near1[base + i] + column(wt_b[i:i + 1]) * o_ref[2 * own + base + i]

    near_ml.wait_recv()
    far_o, far_ml = [], []
    for j in range(n_chunks):
        rows = pl.ds(j * per, per)
        merge_near(0, j)
        far_ml.append(send(nml.at[rows], fml.at[rows], fms.at[j], fmr.at[j], to_chip))
        far_o.append(send(near1.at[rows], far1.at[rows], f1s.at[j], f1r.at[j], to_chip))
        far_ml[j].start()
        far_o[j].start()
    for j in range(n_chunks):
        merge_near(1, j)

    tp_o = []
    for j in range(n_chunks):
        base = j * per
        far_ml[j].wait_recv()
        far_o[j].wait_recv()
        wt_a, wt_b, stat = weights(nml[own + base:own + base + per, :], fml[base:base + per, :])
        inv = pltpu.roll(1.0 / stat, rows_q, 1)
        wt_a, wt_b = wt_a * inv, wt_b * inv
        for i in range(per):
            comb[i * rows_q:(i + 1) * rows_q, :] = (column(wt_a[i:i + 1]) * near1[own + base + i]
                                                    + column(wt_b[i:i + 1]) * far1[base + i])
        for step in range(n_steps):
            for h in range(heads):
                attn[step * per:(step + 1) * per, h * hd:(h + 1) * hd] = comb[pl.ds(step * heads + h, per, stride=rows_q), :]
        attn_in = attn[...].astype(jnp.bfloat16)

        def o_tile(n, carry, j=j, attn_in=attn_in):
            acc = None
            for k in range(k_o):
                if j == 0:
                    arrived(n * k_o + k)
                prod = jnp.dot(attn_in[:, k * kt:(k + 1) * kt], ring[n * k_o + k], preferred_element_type=jnp.float32)
                acc = prod if acc is None else acc + prod
            part_o[j, :, pl.ds(pl.multiple_of(n * nt, nt), nt)] = acc
            return carry
        lax.fori_loop(0, n_o, o_tile, 0)
        tp_o.append(send(part_o.at[j], recv_o.at[j], os_.at[j], or_.at[j], to_tp))
        tp_o[j].start()
    start_many(n_slots, n_slots + first_mlp)

    mid_x = [send(mid_out.at[j], mid_in.at[j], ms_.at[j], mr_.at[j], to_core) for j in range(n_chunks)]

    def pair_d(h, t):
        return send(other_d.at[h, t], other_in.at[h, t], ps_.at[h, t], pr_.at[h, t], to_core)

    def tp_d(h, t):
        return send(part_d.at[h, t], fin.at[h, t], ds_.at[h, t], dr_.at[h, t], to_tp)

    def chip_d(h, t):
        return send(fin.at[h, t], across.at[h, t], xs_.at[h, t], xr_.at[h, t], to_chip)

    def core_d(h, t):
        return send(fin.at[h, t], near.at[h, t], cs_.at[h, t], cr_.at[h, t], to_core)

    def diag_d(h, t):
        return send(across.at[h, t], diag.at[h, t], gs_.at[h, t], gr_.at[h, t], to_core)

    def cols(t):
        return pl.ds(t * nt if isinstance(t, int) else pl.multiple_of(t * nt, nt), nt)

    def emit(who, h, t, value):
        rows = pl.ds(pl.multiple_of(who * n_tok + h * hrows, hrows), hrows)
        out_ref[rows, cols(t)] = value.astype(out_ref.dtype)

    half = 16

    def residual(j):
        tp_o[j].wait_recv()
        h, low = j // 2, (j % 2) * tok

        def norm_rows(i, carry):
            sub = pl.ds(pl.multiple_of(i * half, half), half)
            rows = pl.ds(pl.multiple_of(j * tok + i * half, half), half)
            summed = x_ref[rows, :].astype(jnp.float32) + (part_o[j, sub, :] + recv_o[j, sub, :])
            resid = summed.astype(jnp.bfloat16)
            res[rows, :] = resid
            wide = resid.astype(jnp.float32)
            inv = lax.rsqrt(jnp.mean(wide * wide, axis=-1, keepdims=True) + NORM_EPS)
            scaled = wide * inv * gain_ref[...].astype(jnp.float32)
            mid_out[j, sub, :] = scaled
            mid[h, pl.ds(pl.multiple_of(low + i * half, half), half), :] = scaled.astype(jnp.bfloat16)
            return carry
        lax.fori_loop(0, tok // half, norm_rows, 0)
        mid_x[j].start()

    def partner(j):
        mid_x[j].wait_recv()
        h, low = j // 2, hrows + (j % 2) * tok

        def copy_rows(i, carry):
            sub = pl.ds(pl.multiple_of(i * half, half), half)
            mid[h, pl.ds(pl.multiple_of(low + i * half, half), half), :] = mid_in[j, sub, :].astype(jnp.bfloat16)
            return carry
        lax.fori_loop(0, tok // half, copy_rows, 0)

    def up_tile(h, t):
        idx = first_mlp + h * mlp_loads + 2 * k_up * t
        total = []
        for side in (0, 1):
            acc = None
            for k in range(k_up):
                slot = arrived(idx + side * k_up + k)
                prod = jnp.dot(mid[h, :, k * kt:(k + 1) * kt], ring[slot], preferred_element_type=jnp.float32)
                acc = prod if acc is None else acc + prod
            total.append(acc)
        gate, up = total
        act[:, cols(t)] = (jax.nn.silu(gate) * up).astype(jnp.bfloat16)
        for k in range(2 * k_up):
            start(idx + k + n_slots)

    def down(h, t):
        idx = first_mlp + h * mlp_loads + up_loads + k_dn * t
        acc = None
        for k in range(k_dn):
            slot = arrived(idx + k)
            prod = jnp.dot(act[:, k * kt:(k + 1) * kt], ring[slot], preferred_element_type=jnp.float32)
            acc = prod if acc is None else acc + prod
        part_d[h, t] = acc[:hrows]
        other_d[h, t] = acc[hrows:]
        pair_d(h, t).start()
        for k in range(k_dn):
            start(idx + k + n_slots)

    def reduce(h, t):
        pair_d(h, t).wait_recv()
        part_d[h, t] = part_d[h, t] + other_in[h, t]
        tp_d(h, t).start()

    def finish(h, t):
        tp_d(h, t).wait_recv()
        fin[h, t] = res[h * hrows:(h + 1) * hrows, cols(t)].astype(jnp.float32) + (part_d[h, t] + fin[h, t])
        chip_d(h, t).start()
        core_d(h, t).start()
        emit(sp, h, t, fin[h, t])

    def forward(h, t):
        chip_d(h, t).wait_recv()
        diag_d(h, t).start()
        emit(sp_chip, h, t, across[h, t])
        core_d(h, t).wait_recv()
        emit(sp_core, h, t, near[h, t])

    def collect(h, t):
        diag_d(h, t).wait_recv()
        emit(sp_diag, h, t, diag[h, t])

    def loop(lo, hi, fn):
        def one(t, carry):
            fn(t)
            return carry
        lax.fori_loop(lo, hi, one, 0)

    def down_then_reduce(h):
        def one(t):
            down(h, t)
            reduce(h, t - 1)
        return one

    for j in (0, 1):
        residual(j)
    for j in (0, 1):
        partner(j)
    loop(0, n_up, lambda t: up_tile(0, t))
    down(0, 0)
    loop(1, n_dn, down_then_reduce(0))
    reduce(0, n_dn - 1)

    for j in (2, 3):
        residual(j)
    for j in (2, 3):
        partner(j)
    up_tile(1, 0)

    def up_then_finish(t):
        up_tile(1, t)
        finish(0, t - 1)

    loop(1, n_up, up_then_finish)
    down(1, 0)
    finish(0, n_up - 1)

    def down_more(t):
        down(1, t)
        reduce(1, t - 1)

    loop(1, 3, down_more)
    finish(0, n_up)
    loop(3, 5, down_more)
    finish(0, n_up + 1)
    loop(5, n_dn, down_more)
    reduce(1, n_dn - 1)
    loop(0, n_dn // 2, lambda t: forward(0, t))

    def wind_a(t):
        finish(1, t)
        forward(0, t + n_dn // 2)

    loop(0, n_dn // 2, wind_a)

    def wind_b(t):
        finish(1, t)
        forward(1, t - n_dn // 2)
        collect(0, t - n_dn // 2)

    loop(n_dn // 2, n_dn, wind_b)

    def wind_c(t):
        collect(0, t)
        forward(1, t)
        collect(1, t - n_dn // 2)

    loop(n_dn // 2, n_dn, wind_c)
    loop(n_dn // 2, n_dn, lambda t: collect(1, t))

    for copy in near_o + [near_ml] + far_o + far_ml + tp_o + mid_x:
        copy.wait_send()
    for h in (0, 1):
        for build in (pair_d, tp_d, chip_d, core_d, diag_d):
            loop(0, n_dn, lambda t, h=h, build=build: build(h, t).wait_send())


def finish_layer(o_part, ml, x_own, norm, w_o, w_gate, w_up, w_down, n_steps, heads, exp_scale):
    n_batch, rows_q, hd = o_part.shape
    tokens, width = x_own.shape
    own = tokens // n_steps
    inner = w_gate.shape[1] // 2
    n_chunks, n_slots, kt, nt = 4, 20, 1024, 512
    per = own // n_chunks
    n_dn = width // nt
    vmem = pl.BlockSpec(memory_space=pltpu.VMEM)
    hbm = pl.BlockSpec(memory_space=pl.ANY)
    f32, bf16 = jnp.float32, jnp.bfloat16
    tiles = pltpu.VMEM((2, n_dn, tokens // 2, nt), f32)
    chunk = pltpu.VMEM((n_chunks, per * n_steps, width), f32)
    dma = pltpu.SemaphoreType.DMA
    return pl.pallas_call(
        functools.partial(tail_kernel, (n_steps, heads, hd, n_chunks, exp_scale, n_slots)),
        in_specs=[vmem] * 4 + [hbm] * 4,
        out_specs=vmem,
        out_shape=jax.ShapeDtypeStruct((4 * tokens, width), bf16),
        scratch_shapes=[pltpu.VMEM((n_slots, kt, nt), bf16),
                        pltpu.VMEM((2 * own, rows_q, hd), f32), pltpu.VMEM((2 * own, 2 * rows_q), f32),
                        pltpu.VMEM((own, rows_q, hd), f32), pltpu.VMEM((own, 2 * rows_q), f32),
                        pltpu.VMEM((per * rows_q, hd), f32),
                        pltpu.VMEM((per * n_steps, heads * hd), f32),
                        chunk, chunk,
                        pltpu.VMEM((tokens, width), bf16), pltpu.VMEM((2, tokens, width), bf16), chunk, chunk,
                        pltpu.VMEM((tokens, inner), bf16),
                        tiles, tiles, tiles, tiles, tiles, tiles, tiles,
                        dma((n_slots,)), dma((2 * n_chunks,)), dma((2 * n_chunks,)), dma((1,)), dma((1,)),
                        dma((n_chunks,)), dma((n_chunks,)), dma((n_chunks,)), dma((n_chunks,)), dma((n_chunks,)), dma((n_chunks,)),
                        dma((n_chunks,)), dma((n_chunks,))] + [dma((2, n_dn))] * 10,
        compiler_params=pltpu.CompilerParams(collective_id=0, has_side_effects=True, vmem_limit_bytes=63 * 2**20),
        name="finish_layer",
    )(o_part, ml, x_own, norm.reshape(1, width), w_o, w_gate, w_up, w_down)


def solution(mesh):
    cache_spec = P('dp', 'sp', 'tp', None)
    col_spec = P(None, 'tp')
    row_spec = P('tp', None)
    in_specs = (P(None, 'dp', None), P('dp'), cache_spec, cache_spec, col_spec, col_spec, col_spec, row_spec,
                col_spec, col_spec, row_spec, P(), P(), P(), P())
    out_specs = (P(None, 'dp', None), cache_spec, cache_spec)

    def shard_body(hidden, start_pos, k_cache, v_cache, w_q, w_k, w_v, w_o, w_gate, w_up, w_down, attn_norm, mlp_norm, q_gain, k_gain):
        n_steps, n_batch, width = hidden.shape
        seq_blk, kv_heads, hd = k_cache.shape[1], k_cache.shape[2], k_cache.shape[3]
        heads = w_q.shape[1] // hd
        rows_q = n_steps * heads
        exp_scale = hd ** -0.5 * math.log2(math.e)
        sp = lax.axis_index('sp')
        core, chip = sp % 2, sp // 2
        own = n_batch // 4

        tok_pos = (start_pos[None, :] + jnp.arange(n_steps, dtype=jnp.int32)[:, None]).reshape(-1)
        cos_tab, sin_tab = rope_tables(tok_pos, hd)
        q_rows, k_rows, v_rows = project_qkv(hidden.reshape(n_steps * n_batch, width), attn_norm, cos_tab, sin_tab,
                                             q_gain, k_gain, w_q, w_k, w_v)
        q_rot = q_rows.reshape(n_steps, n_batch, heads, hd)
        k_rows = k_rows.reshape(n_steps, n_batch * kv_heads, hd)
        v_rows = v_rows.reshape(n_steps, n_batch * kv_heads, hd)

        n_req = 4
        per = own // n_req
        part = jnp.stack([(1 - chip) * 2 + (1 - core), chip * 2 + (1 - core), (1 - chip) * 2 + core, chip * 2 + core])
        order = (part[:, None] * per + jnp.arange(per)[None, :]).reshape(-1).astype(jnp.int32)
        rel = start_pos - sp * seq_blk
        flat = (n_batch, seq_blk * kv_heads, hd)
        k_out, v_out, o_part, ml = attention(order, rel, q_rot, k_rows, v_rows, k_cache.reshape(flat), v_cache.reshape(flat),
                                             kv_heads, exp_scale, n_req)

        n_chunks = 4
        per_chunk = own // n_chunks
        x_own = lax.dynamic_slice_in_dim(hidden, sp * own, own, axis=1).reshape(n_steps, n_chunks, per_chunk, width)
        x_own = x_own.transpose(1, 0, 2, 3).reshape(n_steps * own, width)
        flat_out = finish_layer(o_part, ml.reshape(n_batch, 2 * rows_q), x_own, mlp_norm, w_o, w_gate, w_up, w_down,
                                n_steps, heads, exp_scale)
        hid_out = flat_out.reshape(4 * n_chunks, n_steps, per_chunk, width).transpose(1, 0, 2, 3).reshape(n_steps, n_batch, width)
        return hid_out, k_out.reshape(k_cache.shape), v_out.reshape(v_cache.shape)

    return jax.shard_map(shard_body, mesh=mesh, in_specs=in_specs, out_specs=out_specs, check_vma=False)
```

```python
import functools
import math

import jax
import jax.numpy as jnp
from jax import lax
from jax.experimental import pallas as pl
from jax.experimental.pallas import tpu as pltpu
from jax.sharding import PartitionSpec as P

ROPE_BASE = 1000000.0
NORM_EPS = 1e-06
MASKED = -3e38
FLOOR = -1e38


def rms_scale(values, gain_vec):
    wide_vals = values.astype(jnp.float32)
    inv_rms = lax.rsqrt(jnp.mean(wide_vals * wide_vals, axis=-1, keepdims=True) + NORM_EPS)
    return wide_vals * inv_rms * gain_vec.astype(jnp.float32)


def rope_tables(tok_pos, head_dim):
    half_dim = head_dim // 2
    freqs = ROPE_BASE ** (-(jnp.arange(half_dim, dtype=jnp.float32) * (2.0 / head_dim)))
    angles = tok_pos.astype(jnp.float32)[:, None] * freqs[None, :]
    cos_tab = jnp.cos(angles)
    sin_tab = jnp.sin(angles)
    return jnp.concatenate([cos_tab, cos_tab], axis=-1), jnp.concatenate([-sin_tab, sin_tab], axis=-1)


def qkv_kernel(dims, x_ref, norm_ref, cos_ref, sin_ref, qg_ref, kg_ref, wq_hbm, wk_hbm, wv_hbm, q_ref, k_ref, v_ref,
               n_ref, ya_ref, yb_ref, qf_ref, wbuf, sems):
    heads, kv_heads, hd, unit, n_buf = dims
    tokens = x_ref.shape[0]
    rows_blk = 64
    per = unit // hd
    n_q, n_kv = heads // per, kv_heads // per
    total = n_q + 2 * n_kv

    units = [(wk_hbm, g, k_ref, kg_ref) for g in range(n_kv)] + [(wv_hbm, g, v_ref, None) for g in range(n_kv)]
    units += [(wq_hbm, g, qf_ref, qg_ref) for g in range(n_q)]

    def fetch(g):
        hbm, col, _, _ = units[g]
        slot = g % n_buf
        return pltpu.make_async_copy(hbm.at[:, pl.ds(col * unit, unit)], wbuf.at[slot], sems.at[slot])

    for g in range(n_buf - 1):
        fetch(g).start()

    def norm_rows(i, carry):
        rows = pl.ds(pl.multiple_of(i * rows_blk, rows_blk), rows_blk)
        wide = x_ref[rows, :].astype(jnp.float32)
        inv = lax.rsqrt(jnp.mean(wide * wide, axis=-1, keepdims=True) + NORM_EPS)
        n_ref[rows, :] = (wide * inv * norm_ref[...].astype(jnp.float32)).astype(n_ref.dtype)
        return carry

    lax.fori_loop(0, tokens // rows_blk, norm_rows, 0)

    def rotate(vec, rows, gain_ref):
        inv = lax.rsqrt(jnp.mean(vec * vec, axis=-1, keepdims=True) + NORM_EPS)
        vec = vec * inv * gain_ref[...].astype(jnp.float32)
        return vec * cos_ref[rows, :] + pltpu.roll(vec, hd // 2, 1) * sin_ref[rows, :]

    def store(g):
        _, col, dst, gain_ref = units[g]
        y_ref = (ya_ref, yb_ref)[g % 2]
        n_heads = heads if dst is qf_ref else kv_heads
        step = 64
        for low in range(0, tokens, step):
            for h in range(per):
                vec = y_ref[low:low + step, h * hd:(h + 1) * hd]
                if gain_ref is not None:
                    vec = rotate(vec, slice(low, low + step), gain_ref)
                if dst is not qf_ref:
                    vec = vec.astype(jnp.bfloat16).astype(jnp.float32)
                dst[pl.ds(low * n_heads + col * per + h, step, stride=n_heads), :] = vec

    for g in range(total):
        fetch(g).wait()
        for low in range(0, tokens, tokens // 2):
            rows = slice(low, low + tokens // 2)
            (ya_ref, yb_ref)[g % 2][rows, :] = jnp.dot(n_ref[rows, :], wbuf[g % n_buf], preferred_element_type=jnp.float32)
        if g > 0:
            store(g - 1)
        if g + n_buf - 1 < total:
            fetch(g + n_buf - 1).start()
    store(total - 1)

    def cast_rows(i, carry):
        rows = pl.ds(pl.multiple_of(i * 512, 512), 512)
        q_ref[rows, :] = qf_ref[rows, :].astype(q_ref.dtype)
        return carry

    lax.fori_loop(0, tokens * heads // 512, cast_rows, 0)


def project_qkv(x, norm, cos_tab, sin_tab, q_gain, k_gain, w_q, w_k, w_v):
    tokens, width = x.shape
    hd = q_gain.shape[0]
    heads, kv_heads = w_q.shape[1] // hd, w_k.shape[1] // hd
    unit, n_buf = 2 * hd, 4
    vmem = pl.BlockSpec(memory_space=pltpu.VMEM)
    hbm = pl.BlockSpec(memory_space=pl.ANY)
    cols = (heads + 2 * kv_heads) * hd
    return pl.pallas_call(
        functools.partial(qkv_kernel, (heads, kv_heads, hd, unit, n_buf)),
        in_specs=[vmem] * 6 + [hbm] * 3,
        out_specs=[vmem] * 3,
        out_shape=[jax.ShapeDtypeStruct((tokens * heads, hd), jnp.bfloat16),
                   jax.ShapeDtypeStruct((tokens * kv_heads, hd), jnp.float32),
                   jax.ShapeDtypeStruct((tokens * kv_heads, hd), jnp.float32)],
        scratch_shapes=[pltpu.VMEM((tokens, width), jnp.bfloat16),
                        pltpu.VMEM((tokens, unit), jnp.float32),
                        pltpu.VMEM((tokens, unit), jnp.float32),
                        pltpu.VMEM((tokens * heads, hd), jnp.float32),
                        pltpu.VMEM((n_buf, width, unit), jnp.bfloat16),
                        pltpu.SemaphoreType.DMA((n_buf,))],
        compiler_params=pltpu.CompilerParams(vmem_limit_bytes=48 * 2**20),
        cost_estimate=pl.CostEstimate(flops=2 * tokens * width * cols, bytes_accessed=2 * width * cols, transcendentals=0),
        name="project_qkv",
    )(x, norm, cos_tab, sin_tab, q_gain.reshape(1, hd), k_gain.reshape(1, hd), w_q, w_k, w_v)


def attn_kernel(dims, order_ref, rel_ref, q_ref, kn_ref, vn_ref, k_ref, v_ref, ko_ref, vo_ref, o_ref, ml_ref,
                lag_ref, sa_ref, sb_ref, pa_ref, pb_ref):
    n_req, n_steps, heads, kv_heads, groups, rows_c, hd, exp_scale = dims
    rows_q = n_steps * heads
    new_rows = n_steps * kv_heads
    step_rows = 16
    blk = order_ref[pl.program_id(0)]

    @pl.when(pl.program_id(0) == 0)
    def _():
        col = lax.broadcasted_iota(jnp.int32, (rows_q, rows_c), 1)
        row = lax.broadcasted_iota(jnp.int32, (rows_q, rows_c), 0)
        same_head = (col % kv_heads) == ((row % heads) // groups)
        lag_ref[...] = jnp.where(same_head, col // kv_heads - row // heads, jnp.int32(1 << 30))

    win_row = lax.broadcasted_iota(jnp.int32, (2 * new_rows, hd), 0)
    ml_lane = lax.broadcasted_iota(jnp.int32, (step_rows, 2 * rows_q), 1)
    ml_row = lax.broadcasted_iota(jnp.int32, (step_rows, 2 * rows_q), 0)
    pad = jnp.zeros((new_rows, hd), jnp.float32)
    rels = [rel_ref[blk * n_req + j] for j in range(n_req)]

    def insert(j):
        first = rels[j] * kv_heads
        base = pl.multiple_of(jnp.clip((first >> 4) << 4, 0, rows_c - 2 * new_rows), 16)
        off = first - base
        inside = (win_row >= off) & (win_row < off + new_rows)
        for src, new, dst in ((k_ref, kn_ref, ko_ref), (v_ref, vn_ref, vo_ref)):
            dst[j] = src[j]
            fresh = [new[t, j * kv_heads:(j + 1) * kv_heads, :] for t in range(n_steps)]
            rolled = pltpu.roll(jnp.concatenate(fresh + [pad], axis=0), off & (2 * new_rows - 1), 0)
            window = src[j, pl.ds(base, 2 * new_rows), :].astype(jnp.float32)
            dst[j, pl.ds(base, 2 * new_rows), :] = jnp.where(inside, rolled, window).astype(dst.dtype)

    def score(j):
        query = q_ref[:, j].reshape(rows_q, hd)
        (sa_ref, sb_ref)[j % 2][...] = lax.dot_general(query, ko_ref[j], (((1,), (1,)), ((), ())),
                                                       preferred_element_type=jnp.float32)

    def attend(j):
        s_ref, p_ref = ((sa_ref, pa_ref), (sb_ref, pb_ref))[j % 2]
        stats = jnp.zeros((1, 2 * rows_q), jnp.float32)
        for low in range(0, rows_q, step_rows):
            rows = slice(low, low + step_rows)
            scores = jnp.where(lag_ref[rows, :] <= rels[j], s_ref[rows, :], MASKED)
            top = jnp.maximum(jnp.max(scores, axis=1, keepdims=True), FLOOR)
            probs = jnp.exp2((scores - top) * exp_scale)
            total = jnp.sum(probs, axis=1, keepdims=True)
            p_ref[rows, :] = probs.astype(jnp.bfloat16)
            packed = jnp.where(ml_lane == ml_row + low, top, jnp.where(ml_lane == ml_row + (low + rows_q), total, 0.0))
            stats = stats + jnp.sum(packed, axis=0, keepdims=True)
        ml_ref[j] = stats
        o_ref[j] = lax.dot_general(p_ref[...], vo_ref[j], (((1,), (0,)), ((), ())), preferred_element_type=jnp.float32)

    for j in range(n_req):
        insert(j)
    score(0)
    for j in range(n_req):
        if j + 1 < n_req:
            score(j + 1)
        attend(j)


def attention(order, rel, q, k_new, v_new, k_cache, v_cache, kv_heads, exp_scale, n_req=4):
    n_steps, n_batch, heads, hd = q.shape
    rows_c = k_cache.shape[1]
    rows_q = n_steps * heads
    dims = (n_req, n_steps, heads, kv_heads, heads // kv_heads, rows_c, hd, exp_scale)
    cache_blk = pl.BlockSpec((n_req, rows_c, hd), lambda i, order, rel: (order[i], 0, 0))
    new_blk = pl.BlockSpec((n_steps, n_req * kv_heads, hd), lambda i, order, rel: (0, order[i], 0))
    cache_shape = jax.ShapeDtypeStruct(k_cache.shape, k_cache.dtype)
    return pl.pallas_call(
        functools.partial(attn_kernel, dims),
        grid_spec=pltpu.PrefetchScalarGridSpec(
            num_scalar_prefetch=2,
            grid=(n_batch // n_req,),
            in_specs=[pl.BlockSpec((n_steps, n_req, heads, hd), lambda i, order, rel: (0, order[i], 0, 0)),
                      new_blk, new_blk, cache_blk, cache_blk],
            out_specs=[cache_blk, cache_blk,
                       pl.BlockSpec((n_req, rows_q, hd), lambda i, order, rel: (i, 0, 0)),
                       pl.BlockSpec((n_req, 1, 2 * rows_q), lambda i, order, rel: (i, 0, 0))],
            scratch_shapes=[pltpu.VMEM((rows_q, rows_c), jnp.int32)] + [pltpu.VMEM((rows_q, rows_c), jnp.float32)] * 2
                           + [pltpu.VMEM((rows_q, rows_c), jnp.bfloat16)] * 2,
        ),
        out_shape=[cache_shape, cache_shape,
                   jax.ShapeDtypeStruct((n_batch, rows_q, hd), jnp.float32),
                   jax.ShapeDtypeStruct((n_batch, 1, 2 * rows_q), jnp.float32)],
        compiler_params=pltpu.CompilerParams(dimension_semantics=("arbitrary",), vmem_limit_bytes=62 * 2**20),
        cost_estimate=pl.CostEstimate(flops=4 * n_batch * rows_q * rows_c * hd, bytes_accessed=8 * n_batch * rows_c * hd,
                                      transcendentals=n_batch * rows_q * rows_c),
        name="decode_attention",
    )(order, rel, q, k_new, v_new, k_cache, v_cache)


def tail_kernel(dims, o_hbm, ml_hbm, x_hbm, gain_ref, wo_hbm, wg_hbm, wu_hbm, wd_hbm, out_ref,
                ring, o_ref, ml_ref, x_ref, near1, nml, far1, fml, comb, attn, part_o, recv_o, res, mid, mid_out, mid_in, act,
                part_d, other_d, other_in, fin, across, near, diag,
                ring_sem, om_sem, mm_sem, x_sem, n1s, n1r, nms, nmr, f1s, f1r, fms, fmr, os_, or_, ms_, mr_, ps_, pr_, ds_, dr_, xs_, xr_, cs_, cr_, gs_, gr_):
    n_steps, heads, hd, n_chunks, exp_scale, n_slots = dims
    rows_q = n_steps * heads
    own = far1.shape[0]
    per = own // n_chunks
    tok = per * n_steps
    n_tok, width = res.shape
    hrows = n_tok // 2
    kt, nt = ring.shape[1], ring.shape[2]
    inner = act.shape[1]
    n_o, k_o = width // nt, heads * hd // kt
    n_up, k_up = inner // nt, width // kt
    n_dn, k_dn = width // nt, inner // kt
    first_mlp = n_o * k_o
    up_loads, dn_loads = 2 * k_up * n_up, k_dn * n_dn
    mlp_loads = up_loads + dn_loads
    n_loads = first_mlp + 2 * mlp_loads

    sp = lax.axis_index('sp')
    tp = lax.axis_index('tp')
    core = lax.rem(sp, 2)
    sp_core = sp + 1 - 2 * core
    sp_chip = lax.rem(sp + 2, 4)
    sp_diag = lax.rem(sp_core + 2, 4)
    to_core = {'sp': sp_core}
    to_chip = {'sp': sp_chip}
    to_tp = {'tp': 1 - tp}

    def send(src, dst, s_sem, r_sem, dev):
        return pltpu.make_async_remote_copy(src_ref=src, dst_ref=dst, send_sem=s_sem, recv_sem=r_sem, device_id=dev,
                                            device_id_type=pl.DeviceIdType.MESH)

    barrier = pltpu.get_barrier_semaphore()
    for dev in (to_core, to_chip, to_tp):
        pl.semaphore_signal(barrier, inc=1, device_id=dev, device_id_type=pl.DeviceIdType.MESH)
    pl.semaphore_wait(barrier, 3)

    near_ml = send(ml_hbm.at[pl.ds(0, 2 * own)], nml, nms.at[0], nmr.at[0], to_core)
    near_ml.start()
    near_o = []
    for piece in (0, 1):
        for j in range(n_chunks):
            rows = pl.ds(piece * own + j * per, per)
            near_o.append(send(o_hbm.at[rows], near1.at[rows], n1s.at[piece * n_chunks + j], n1r.at[piece * n_chunks + j], to_core))
    for copy in near_o:
        copy.start()
    mine_ml = pltpu.make_async_copy(ml_hbm.at[pl.ds(2 * own, 2 * own)], ml_ref, mm_sem.at[0])
    mine_ml.start()
    mine_o = [pltpu.make_async_copy(o_hbm.at[pl.ds((2 + piece) * own, own)], o_ref.at[pl.ds(piece * own, own)], om_sem.at[piece])
              for piece in (0, 1)]
    mine_o[0].start()
    mine_o[1].start()

    def load_x(j, step):
        return pltpu.make_async_copy(x_hbm.at[step, pl.ds(pl.multiple_of(sp * own + j * per, per), per)], x_ref.at[j * n_steps + step],
                                     x_sem.at[j * n_steps + step])

    for j in range(n_chunks):
        for step in range(n_steps):
            load_x(j, step).start()

    def load(src, row, col, slot):
        return pltpu.make_async_copy(src.at[pl.ds(pl.multiple_of(row, kt), kt), pl.ds(pl.multiple_of(col, nt), nt)],
                                     ring.at[slot], ring_sem.at[slot])

    def start(idx):
        slot = lax.rem(idx, n_slots)

        @pl.when(idx < first_mlp)
        def _():
            load(wo_hbm, lax.rem(idx, k_o) * kt, (idx // k_o) * nt, slot).start()

        loc = lax.rem(idx - first_mlp + mlp_loads, mlp_loads)
        in_mlp = (idx >= first_mlp) & (idx < n_loads)
        sub = lax.rem(loc, 2 * k_up)
        up_col = core * inner + (loc // (2 * k_up)) * nt

        @pl.when(in_mlp & (loc < up_loads) & (sub < k_up))
        def _():
            load(wg_hbm, sub * kt, up_col, slot).start()

        @pl.when(in_mlp & (loc < up_loads) & (sub >= k_up))
        def _():
            load(wu_hbm, (sub - k_up) * kt, up_col, slot).start()

        dn = loc - up_loads

        @pl.when(in_mlp & (loc >= up_loads))
        def _():
            load(wd_hbm, core * inner + lax.rem(dn, k_dn) * kt, (dn // k_dn) * nt, slot).start()

    def arrived(idx):
        slot = lax.rem(idx, n_slots)
        load(wo_hbm, 0, 0, slot).wait()
        return slot

    def start_many(lo, hi):
        def one(i, carry):
            start(i)
            return carry
        lax.fori_loop(lo, hi, one, 0)

    start_many(0, n_slots)

    diag_mask = lax.broadcasted_iota(jnp.int32, (rows_q, 2 * rows_q), 0) == lax.broadcasted_iota(jnp.int32, (rows_q, 2 * rows_q), 1)
    left = lax.broadcasted_iota(jnp.int32, (per, 2 * rows_q), 1) < rows_q

    def column(row):
        return jnp.sum(jnp.where(diag_mask, row, 0.0), axis=1, keepdims=True)

    def weights(stat_a, stat_b):
        top = jnp.maximum(stat_a, stat_b)
        wt_a = jnp.exp2((stat_a - top) * exp_scale)
        wt_b = jnp.exp2((stat_b - top) * exp_scale)
        total = pltpu.roll(wt_a, rows_q, 1) * stat_a + pltpu.roll(wt_b, rows_q, 1) * stat_b
        return wt_a, wt_b, jnp.where(left, top, total)

    def merge_near(piece, j):
        base = piece * own + j * per
        near_o[piece * n_chunks + j].wait_recv()
        wt_a, wt_b, stat = weights(nml[base:base + per, :], ml_ref[base:base + per, :])
        nml[base:base + per, :] = stat
        for i in range(per):
            near1[base + i] = column(wt_a[i:i + 1]) * near1[base + i] + column(wt_b[i:i + 1]) * o_ref[base + i]

    near_ml.wait_recv()
    mine_ml.wait()
    mine_o[0].wait()
    far_o, far_ml = [], []
    for j in range(n_chunks):
        rows = pl.ds(j * per, per)
        merge_near(0, j)
        far_ml.append(send(nml.at[rows], fml.at[rows], fms.at[j], fmr.at[j], to_chip))
        far_o.append(send(near1.at[rows], far1.at[rows], f1s.at[j], f1r.at[j], to_chip))
        far_ml[j].start()
        far_o[j].start()
    mine_o[1].wait()
    for j in range(n_chunks):
        merge_near(1, j)

    def tp_o(j, n):
        return send(part_o.at[j, n], recv_o.at[j, n], os_.at[j, n], or_.at[j, n], to_tp)

    for j in range(n_chunks):
        base = j * per
        far_ml[j].wait_recv()
        far_o[j].wait_recv()
        wt_a, wt_b, stat = weights(nml[own + base:own + base + per, :], fml[base:base + per, :])
        inv = pltpu.roll(1.0 / stat, rows_q, 1)
        wt_a, wt_b = wt_a * inv, wt_b * inv
        for i in range(per):
            comb[i * rows_q:(i + 1) * rows_q, :] = (column(wt_a[i:i + 1]) * near1[own + base + i]
                                                    + column(wt_b[i:i + 1]) * far1[base + i])
        for step in range(n_steps):
            for h in range(heads):
                attn[step * per:(step + 1) * per, h * hd:(h + 1) * hd] = comb[pl.ds(step * heads + h, per, stride=rows_q), :]
        attn_in = attn[...].astype(jnp.bfloat16)

        def o_tile(n, carry, j=j, attn_in=attn_in):
            acc = None
            for k in range(k_o):
                if j == 0:
                    arrived(n * k_o + k)
                prod = jnp.dot(attn_in[:, k * kt:(k + 1) * kt], ring[n * k_o + k], preferred_element_type=jnp.float32)
                acc = prod if acc is None else acc + prod
            part_o[j, n] = acc
            tp_o(j, n).start()
            return carry
        lax.fori_loop(0, n_o, o_tile, 0)
    start_many(n_slots, n_slots + first_mlp)

    mid_x = [send(mid_out.at[j], mid_in.at[j], ms_.at[j], mr_.at[j], to_core) for j in range(n_chunks)]

    def pair_d(h, t):
        return send(other_d.at[h, t], other_in.at[h, t], ps_.at[h, t], pr_.at[h, t], to_core)

    def tp_d(h, t):
        return send(part_d.at[h, t], fin.at[h, t], ds_.at[h, t], dr_.at[h, t], to_tp)

    def chip_d(h, t):
        return send(fin.at[h, t], across.at[h, t], xs_.at[h, t], xr_.at[h, t], to_chip)

    def core_d(h, t):
        return send(fin.at[h, t], near.at[h, t], cs_.at[h, t], cr_.at[h, t], to_core)

    def diag_d(h, t):
        return send(across.at[h, t], diag.at[h, t], gs_.at[h, t], gr_.at[h, t], to_core)

    def cols(t):
        return pl.ds(t * nt if isinstance(t, int) else pl.multiple_of(t * nt, nt), nt)

    def emit(who, h, t, value):
        for c in (0, 1):
            for step in range(n_steps):
                low = c * tok + step * per
                out_ref[step * 4 * n_chunks + who * n_chunks + 2 * h + c, :, cols(t)] = value[low:low + per].astype(out_ref.dtype)

    def loop(lo, hi, fn):
        def one(t, carry):
            fn(t)
            return carry
        lax.fori_loop(lo, hi, one, 0)

    half = 16

    def residual(j):
        for step in range(n_steps):
            load_x(j, step).wait()
        loop(0, n_o, lambda n: tp_o(j, n).wait_recv())
        h, low = j // 2, (j % 2) * tok

        def norm_rows(i, carry):
            sub = pl.ds(pl.multiple_of(i * half, half), half)
            rows = pl.ds(pl.multiple_of(j * tok + i * half, half), half)
            base = j * n_steps + i * (half // per)
            x_rows = jnp.concatenate([x_ref[base + g].astype(jnp.float32) for g in range(half // per)], axis=0)
            proj = jnp.concatenate([part_o[j, n, sub, :] + recv_o[j, n, sub, :] for n in range(n_o)], axis=1)
            summed = x_rows + proj
            resid = summed.astype(jnp.bfloat16)
            res[rows, :] = resid
            wide = resid.astype(jnp.float32)
            inv = lax.rsqrt(jnp.mean(wide * wide, axis=-1, keepdims=True) + NORM_EPS)
            scaled = wide * inv * gain_ref[...].astype(jnp.float32)
            mid_out[j, sub, :] = scaled
            mid[h, pl.ds(pl.multiple_of(low + i * half, half), half), :] = scaled.astype(jnp.bfloat16)
            return carry
        lax.fori_loop(0, tok // half, norm_rows, 0)
        mid_x[j].start()

    def partner(j):
        mid_x[j].wait_recv()
        h, low = j // 2, hrows + (j % 2) * tok

        def copy_rows(i, carry):
            sub = pl.ds(pl.multiple_of(i * half, half), half)
            mid[h, pl.ds(pl.multiple_of(low + i * half, half), half), :] = mid_in[j, sub, :].astype(jnp.bfloat16)
            return carry
        lax.fori_loop(0, tok // half, copy_rows, 0)

    def up_tile(h, t):
        idx = first_mlp + h * mlp_loads + 2 * k_up * t
        total = []
        for side in (0, 1):
            acc = None
            for k in range(k_up):
                slot = arrived(idx + side * k_up + k)
                prod = jnp.dot(mid[h, :, k * kt:(k + 1) * kt], ring[slot], preferred_element_type=jnp.float32)
                acc = prod if acc is None else acc + prod
            total.append(acc)
        gate, up = total
        act[:, cols(t)] = (jax.nn.silu(gate) * up).astype(jnp.bfloat16)
        for k in range(2 * k_up):
            start(idx + k + n_slots)

    def down(h, t):
        idx = first_mlp + h * mlp_loads + up_loads + k_dn * t
        acc = None
        for k in range(k_dn):
            slot = arrived(idx + k)
            prod = jnp.dot(act[:, k * kt:(k + 1) * kt], ring[slot], preferred_element_type=jnp.float32)
            acc = prod if acc is None else acc + prod
        part_d[h, t] = acc[:hrows]
        other_d[h, t] = acc[hrows:]
        pair_d(h, t).start()
        for k in range(k_dn):
            start(idx + k + n_slots)

    def reduce(h, t):
        pair_d(h, t).wait_recv()
        part_d[h, t] = part_d[h, t] + other_in[h, t]
        tp_d(h, t).start()

    def finish(h, t):
        tp_d(h, t).wait_recv()
        fin[h, t] = res[h * hrows:(h + 1) * hrows, cols(t)].astype(jnp.float32) + (part_d[h, t] + fin[h, t])
        chip_d(h, t).start()
        core_d(h, t).start()
        emit(sp, h, t, fin[h, t])

    def forward(h, t):
        chip_d(h, t).wait_recv()
        diag_d(h, t).start()
        emit(sp_chip, h, t, across[h, t])
        core_d(h, t).wait_recv()
        emit(sp_core, h, t, near[h, t])

    def collect(h, t):
        diag_d(h, t).wait_recv()
        emit(sp_diag, h, t, diag[h, t])

    def down_then_reduce(h):
        def one(t):
            down(h, t)
            reduce(h, t - 1)
        return one

    for j in (0, 1):
        residual(j)
    for j in (0, 1):
        partner(j)
    loop(0, n_up, lambda t: up_tile(0, t))
    down(0, 0)
    loop(1, n_dn, down_then_reduce(0))
    reduce(0, n_dn - 1)

    for j in (2, 3):
        residual(j)
    for j in (2, 3):
        partner(j)
    up_tile(1, 0)

    def up_then_finish(t):
        up_tile(1, t)
        finish(0, t - 1)

    loop(1, n_up, up_then_finish)
    down(1, 0)
    finish(0, n_up - 1)

    def down_more(t):
        down(1, t)
        reduce(1, t - 1)

    loop(1, 3, down_more)
    finish(0, n_up)
    loop(3, 5, down_more)
    finish(0, n_up + 1)
    loop(5, n_dn, down_more)
    reduce(1, n_dn - 1)
    loop(0, n_dn // 2, lambda t: forward(0, t))

    def wind_a(t):
        finish(1, t)
        forward(0, t + n_dn // 2)

    loop(0, n_dn // 2, wind_a)

    def wind_b(t):
        finish(1, t)
        forward(1, t - n_dn // 2)
        collect(0, t - n_dn // 2)

    loop(n_dn // 2, n_dn, wind_b)

    def wind_c(t):
        collect(0, t)
        forward(1, t)
        collect(1, t - n_dn // 2)

    loop(n_dn // 2, n_dn, wind_c)
    loop(n_dn // 2, n_dn, lambda t: collect(1, t))

    for copy in near_o + [near_ml] + far_o + far_ml + mid_x:
        copy.wait_send()
    for j in range(n_chunks):
        loop(0, n_o, lambda n, j=j: tp_o(j, n).wait_send())
    for h in (0, 1):
        for build in (pair_d, tp_d, chip_d, core_d, diag_d):
            loop(0, n_dn, lambda t, h=h, build=build: build(h, t).wait_send())


def finish_layer(o_part, ml, hidden, norm, w_o, w_gate, w_up, w_down, heads, exp_scale):
    n_batch, rows_q, hd = o_part.shape
    n_steps, _, width = hidden.shape
    own = n_batch // 4
    tokens = own * n_steps
    inner = w_gate.shape[1] // 2
    n_chunks, n_slots, kt, nt = 4, 20, 1024, 512
    per = own // n_chunks
    n_dn = width // nt
    vmem = pl.BlockSpec(memory_space=pltpu.VMEM)
    hbm = pl.BlockSpec(memory_space=pl.ANY)
    f32, bf16 = jnp.float32, jnp.bfloat16
    tiles = pltpu.VMEM((2, n_dn, tokens // 2, nt), f32)
    chunk = pltpu.VMEM((n_chunks, per * n_steps, width), f32)
    o_tiles = pltpu.VMEM((n_chunks, n_dn, per * n_steps, nt), f32)
    dma = pltpu.SemaphoreType.DMA
    return pl.pallas_call(
        functools.partial(tail_kernel, (n_steps, heads, hd, n_chunks, exp_scale, n_slots)),
        in_specs=[hbm] * 3 + [vmem] + [hbm] * 4,
        out_specs=vmem,
        out_shape=jax.ShapeDtypeStruct((n_steps * n_batch // per, per, width), bf16),
        scratch_shapes=[pltpu.VMEM((n_slots, kt, nt), bf16),
                        pltpu.VMEM((2 * own, rows_q, hd), f32), pltpu.VMEM((2 * own, 2 * rows_q), f32),
                        pltpu.VMEM((n_chunks * n_steps, per, width), bf16),
                        pltpu.VMEM((2 * own, rows_q, hd), f32), pltpu.VMEM((2 * own, 2 * rows_q), f32),
                        pltpu.VMEM((own, rows_q, hd), f32), pltpu.VMEM((own, 2 * rows_q), f32),
                        pltpu.VMEM((per * rows_q, hd), f32),
                        pltpu.VMEM((per * n_steps, heads * hd), f32),
                        o_tiles, o_tiles,
                        pltpu.VMEM((tokens, width), bf16), pltpu.VMEM((2, tokens, width), bf16), chunk, chunk,
                        pltpu.VMEM((tokens, inner), bf16),
                        tiles, tiles, tiles, tiles, tiles, tiles, tiles,
                        dma((n_slots,)), dma((2,)), dma((1,)), dma((n_chunks * n_steps,)),
                        dma((2 * n_chunks,)), dma((2 * n_chunks,)), dma((1,)), dma((1,)),
                        dma((n_chunks,)), dma((n_chunks,)), dma((n_chunks,)), dma((n_chunks,)), dma((n_chunks, n_dn)), dma((n_chunks, n_dn)),
                        dma((n_chunks,)), dma((n_chunks,))] + [dma((2, n_dn))] * 10,
        compiler_params=pltpu.CompilerParams(collective_id=0, has_side_effects=True, vmem_limit_bytes=63 * 2**20),
        name="finish_layer",
    )(o_part, ml, hidden, norm, w_o, w_gate, w_up, w_down)


def solution(mesh):
    cache_spec = P('dp', 'sp', 'tp', None)
    col_spec = P(None, 'tp')
    row_spec = P('tp', None)
    in_specs = (P(None, 'dp', None), P('dp'), cache_spec, cache_spec, col_spec, col_spec, col_spec, row_spec,
                col_spec, col_spec, row_spec, P(), P(), P(), P())
    out_specs = (P(None, 'dp', None), cache_spec, cache_spec)

    def shard_body(hidden, start_pos, k_cache, v_cache, w_q, w_k, w_v, w_o, w_gate, w_up, w_down, attn_norm, mlp_norm, q_gain, k_gain):
        n_steps, n_batch, width = hidden.shape
        seq_blk, kv_heads, hd = k_cache.shape[1], k_cache.shape[2], k_cache.shape[3]
        heads = w_q.shape[1] // hd
        rows_q = n_steps * heads
        exp_scale = hd ** -0.5 * math.log2(math.e)
        sp = lax.axis_index('sp')
        core, chip = sp % 2, sp // 2
        own = n_batch // 4

        tok_pos = (start_pos[None, :] + jnp.arange(n_steps, dtype=jnp.int32)[:, None]).reshape(-1)
        cos_tab, sin_tab = rope_tables(tok_pos, hd)
        norms = jnp.stack([attn_norm, mlp_norm]).astype(jnp.float32)
        q_rows, k_rows, v_rows = project_qkv(hidden.reshape(n_steps * n_batch, width), norms[:1], cos_tab, sin_tab,
                                             q_gain, k_gain, w_q, w_k, w_v)
        q_rot = q_rows.reshape(n_steps, n_batch, heads, hd)
        k_rows = k_rows.reshape(n_steps, n_batch * kv_heads, hd)
        v_rows = v_rows.reshape(n_steps, n_batch * kv_heads, hd)

        n_req = 8
        per = own // n_req
        part = jnp.stack([(1 - chip) * 2 + (1 - core), chip * 2 + (1 - core), (1 - chip) * 2 + core, chip * 2 + core])
        order = (part[:, None] * per + jnp.arange(per)[None, :]).reshape(-1).astype(jnp.int32)
        rel = start_pos - sp * seq_blk
        flat = (n_batch, seq_blk * kv_heads, hd)
        k_out, v_out, o_part, ml = attention(order, rel, q_rot, k_rows, v_rows, k_cache.reshape(flat), v_cache.reshape(flat),
                                             kv_heads, exp_scale, n_req)

        hid_out = finish_layer(o_part, ml.reshape(n_batch, 2 * rows_q), hidden, norms[1:], w_o, w_gate, w_up, w_down,
                               heads, exp_scale).reshape(hidden.shape)
        return hid_out, k_out.reshape(k_cache.shape), v_out.reshape(v_cache.shape)

    return jax.shard_map(shard_body, mesh=mesh, in_specs=in_specs, out_specs=out_specs, check_vma=False)
```

```python
import functools
import math

import jax
import jax.numpy as jnp
from jax import lax
from jax.experimental import pallas as pl
from jax.experimental.pallas import tpu as pltpu
from jax.sharding import PartitionSpec as P

ROPE_BASE = 1000000.0
NORM_EPS = 1e-06
MASKED = -3e38
FLOOR = -1e38


def rms_scale(values, gain_vec):
    wide_vals = values.astype(jnp.float32)
    inv_rms = lax.rsqrt(jnp.mean(wide_vals * wide_vals, axis=-1, keepdims=True) + NORM_EPS)
    return wide_vals * inv_rms * gain_vec.astype(jnp.float32)


def rope_tables(tok_pos, head_dim):
    half_dim = head_dim // 2
    freqs = ROPE_BASE ** (-(jnp.arange(half_dim, dtype=jnp.float32) * (2.0 / head_dim)))
    angles = tok_pos.astype(jnp.float32)[:, None] * freqs[None, :]
    cos_tab = jnp.cos(angles)
    sin_tab = jnp.sin(angles)
    return jnp.concatenate([cos_tab, cos_tab], axis=-1), jnp.concatenate([-sin_tab, sin_tab], axis=-1)


def qkv_kernel(dims, x_ref, norm_ref, cos_ref, sin_ref, qg_ref, kg_ref, wq_hbm, wk_hbm, wv_hbm, q_ref, k_ref, v_ref,
               n_ref, ya_ref, yb_ref, qf_ref, wbuf, sems):
    heads, kv_heads, hd, unit, n_buf = dims
    tokens = x_ref.shape[0]
    rows_blk = 64
    per = unit // hd
    n_q, n_kv = heads // per, kv_heads // per
    total = n_q + 2 * n_kv

    units = [(wk_hbm, g, k_ref, kg_ref) for g in range(n_kv)] + [(wv_hbm, g, v_ref, None) for g in range(n_kv)]
    units += [(wq_hbm, g, qf_ref, qg_ref) for g in range(n_q)]

    def fetch(g):
        hbm, col, _, _ = units[g]
        slot = g % n_buf
        return pltpu.make_async_copy(hbm.at[:, pl.ds(col * unit, unit)], wbuf.at[slot], sems.at[slot])

    for g in range(n_buf - 1):
        fetch(g).start()

    def norm_rows(i, carry):
        rows = pl.ds(pl.multiple_of(i * rows_blk, rows_blk), rows_blk)
        wide = x_ref[rows, :].astype(jnp.float32)
        inv = lax.rsqrt(jnp.mean(wide * wide, axis=-1, keepdims=True) + NORM_EPS)
        n_ref[rows, :] = (wide * inv * norm_ref[...].astype(jnp.float32)).astype(n_ref.dtype)
        return carry

    lax.fori_loop(0, tokens // rows_blk, norm_rows, 0)

    def rotate(vec, rows, gain_ref):
        inv = lax.rsqrt(jnp.mean(vec * vec, axis=-1, keepdims=True) + NORM_EPS)
        vec = vec * inv * gain_ref[...].astype(jnp.float32)
        return vec * cos_ref[rows, :] + pltpu.roll(vec, hd // 2, 1) * sin_ref[rows, :]

    def store(g):
        _, col, dst, gain_ref = units[g]
        y_ref = (ya_ref, yb_ref)[g % 2]
        n_heads = heads if dst is qf_ref else kv_heads
        step = 64
        for low in range(0, tokens, step):
            for h in range(per):
                vec = y_ref[low:low + step, h * hd:(h + 1) * hd]
                if gain_ref is not None:
                    vec = rotate(vec, slice(low, low + step), gain_ref)
                if dst is not qf_ref:
                    vec = vec.astype(jnp.bfloat16).astype(jnp.float32)
                dst[pl.ds(low * n_heads + col * per + h, step, stride=n_heads), :] = vec

    for g in range(total):
        fetch(g).wait()
        for low in range(0, tokens, tokens // 2):
            rows = slice(low, low + tokens // 2)
            (ya_ref, yb_ref)[g % 2][rows, :] = jnp.dot(n_ref[rows, :], wbuf[g % n_buf], preferred_element_type=jnp.float32)
        if g > 0:
            store(g - 1)
        if g + n_buf - 1 < total:
            fetch(g + n_buf - 1).start()
    store(total - 1)

    def cast_rows(i, carry):
        rows = pl.ds(pl.multiple_of(i * 512, 512), 512)
        q_ref[rows, :] = qf_ref[rows, :].astype(q_ref.dtype)
        return carry

    lax.fori_loop(0, tokens * heads // 512, cast_rows, 0)


def project_qkv(x, norm, cos_tab, sin_tab, q_gain, k_gain, w_q, w_k, w_v):
    tokens, width = x.shape
    hd = q_gain.shape[0]
    heads, kv_heads = w_q.shape[1] // hd, w_k.shape[1] // hd
    unit, n_buf = 2 * hd, 4
    vmem = pl.BlockSpec(memory_space=pltpu.VMEM)
    hbm = pl.BlockSpec(memory_space=pl.ANY)
    cols = (heads + 2 * kv_heads) * hd
    return pl.pallas_call(
        functools.partial(qkv_kernel, (heads, kv_heads, hd, unit, n_buf)),
        in_specs=[vmem] * 6 + [hbm] * 3,
        out_specs=[vmem] * 3,
        out_shape=[jax.ShapeDtypeStruct((tokens * heads, hd), jnp.bfloat16),
                   jax.ShapeDtypeStruct((tokens * kv_heads, hd), jnp.float32),
                   jax.ShapeDtypeStruct((tokens * kv_heads, hd), jnp.float32)],
        scratch_shapes=[pltpu.VMEM((tokens, width), jnp.bfloat16),
                        pltpu.VMEM((tokens, unit), jnp.float32),
                        pltpu.VMEM((tokens, unit), jnp.float32),
                        pltpu.VMEM((tokens * heads, hd), jnp.float32),
                        pltpu.VMEM((n_buf, width, unit), jnp.bfloat16),
                        pltpu.SemaphoreType.DMA((n_buf,))],
        compiler_params=pltpu.CompilerParams(vmem_limit_bytes=62 * 2**20),
        cost_estimate=pl.CostEstimate(flops=2 * tokens * width * cols, bytes_accessed=2 * width * cols, transcendentals=0),
        name="project_qkv",
    )(x, norm, cos_tab, sin_tab, q_gain.reshape(1, hd), k_gain.reshape(1, hd), w_q, w_k, w_v)


def attn_kernel(dims, order_ref, rel_ref, q_ref, kn_ref, vn_ref, k_hbm, v_hbm, ko_ref, vo_ref, o_ref, ml_ref,
                lag_ref, sa_ref, sb_ref, pa_ref, pb_ref, k_buf, v_buf, sems):
    n_req, n_steps, heads, kv_heads, groups, rows_c, hd, exp_scale = dims
    rows_q = n_steps * heads
    new_rows = n_steps * kv_heads
    step_rows = 16
    n_buf = k_buf.shape[0]
    here = pl.program_id(0)
    last = pl.num_programs(0)
    blk = order_ref[here]
    k_ref, v_ref = k_buf.at[lax.rem(here, n_buf)], v_buf.at[lax.rem(here, n_buf)]

    def fetch(step):
        slot = lax.rem(step, n_buf)
        reqs = pl.ds(order_ref[step] * n_req, n_req)
        return (pltpu.make_async_copy(k_hbm.at[reqs], k_buf.at[slot], sems.at[0, slot]),
                pltpu.make_async_copy(v_hbm.at[reqs], v_buf.at[slot], sems.at[1, slot]))

    def begin(step):
        for copy in fetch(step):
            copy.start()

    @pl.when(here == 0)
    def _():
        for step in range(n_buf - 1):
            begin(jnp.int32(step))

    @pl.when(here + n_buf - 1 < last)
    def _():
        begin(here + n_buf - 1)


    @pl.when(pl.program_id(0) == 0)
    def _():
        col = lax.broadcasted_iota(jnp.int32, (rows_q, rows_c), 1)
        row = lax.broadcasted_iota(jnp.int32, (rows_q, rows_c), 0)
        same_head = (col % kv_heads) == ((row % heads) // groups)
        lag_ref[...] = jnp.where(same_head, col // kv_heads - row // heads, jnp.int32(1 << 30))

    win_row = lax.broadcasted_iota(jnp.int32, (2 * new_rows, hd), 0)
    ml_lane = lax.broadcasted_iota(jnp.int32, (step_rows, 2 * rows_q), 1)
    ml_row = lax.broadcasted_iota(jnp.int32, (step_rows, 2 * rows_q), 0)
    pad = jnp.zeros((new_rows, hd), jnp.float32)
    rels = [rel_ref[blk * n_req + j] for j in range(n_req)]

    def insert(j):
        first = rels[j] * kv_heads
        base = pl.multiple_of(jnp.clip((first >> 4) << 4, 0, rows_c - 2 * new_rows), 16)
        off = first - base
        inside = (win_row >= off) & (win_row < off + new_rows)
        for src, new, dst in ((k_ref, kn_ref, ko_ref), (v_ref, vn_ref, vo_ref)):
            dst[j] = src[j]
            fresh = [new[t, j * kv_heads:(j + 1) * kv_heads, :] for t in range(n_steps)]
            rolled = pltpu.roll(jnp.concatenate(fresh + [pad], axis=0), off & (2 * new_rows - 1), 0)
            window = src[j, pl.ds(base, 2 * new_rows), :].astype(jnp.float32)
            dst[j, pl.ds(base, 2 * new_rows), :] = jnp.where(inside, rolled, window).astype(dst.dtype)

    def score(j):
        query = q_ref[:, j].reshape(rows_q, hd)
        (sa_ref, sb_ref)[j % 2][...] = lax.dot_general(query, ko_ref[j], (((1,), (1,)), ((), ())),
                                                       preferred_element_type=jnp.float32)

    def attend(j):
        s_ref, p_ref = ((sa_ref, pa_ref), (sb_ref, pb_ref))[j % 2]
        stats = jnp.zeros((1, 2 * rows_q), jnp.float32)
        for low in range(0, rows_q, step_rows):
            rows = slice(low, low + step_rows)
            scores = jnp.where(lag_ref[rows, :] <= rels[j], s_ref[rows, :], MASKED)
            top = jnp.maximum(jnp.max(scores, axis=1, keepdims=True), FLOOR)
            probs = jnp.exp2((scores - top) * exp_scale)
            total = jnp.sum(probs, axis=1, keepdims=True)
            p_ref[rows, :] = probs.astype(jnp.bfloat16)
            packed = jnp.where(ml_lane == ml_row + low, top, jnp.where(ml_lane == ml_row + (low + rows_q), total, 0.0))
            stats = stats + jnp.sum(packed, axis=0, keepdims=True)
        ml_ref[j] = stats
        o_ref[j] = lax.dot_general(p_ref[...], vo_ref[j], (((1,), (0,)), ((), ())), preferred_element_type=jnp.float32)

    for copy in fetch(here):
        copy.wait()
    for j in range(n_req):
        insert(j)
    score(0)
    for j in range(n_req):
        if j + 1 < n_req:
            score(j + 1)
        attend(j)


def attention(order, rel, q, k_new, v_new, k_cache, v_cache, kv_heads, exp_scale, n_req=4):
    n_steps, n_batch, heads, hd = q.shape
    rows_c = k_cache.shape[1]
    rows_q = n_steps * heads
    dims = (n_req, n_steps, heads, kv_heads, heads // kv_heads, rows_c, hd, exp_scale)
    cache_blk = pl.BlockSpec((n_req, rows_c, hd), lambda i, order, rel: (order[i], 0, 0))
    cache_in = pl.BlockSpec(memory_space=pl.ANY)
    n_buf = 4
    cache_buf = pltpu.VMEM((n_buf, n_req, rows_c, hd), k_cache.dtype)
    new_blk = pl.BlockSpec((n_steps, n_req * kv_heads, hd), lambda i, order, rel: (0, order[i], 0))
    cache_shape = jax.ShapeDtypeStruct(k_cache.shape, k_cache.dtype)
    return pl.pallas_call(
        functools.partial(attn_kernel, dims),
        grid_spec=pltpu.PrefetchScalarGridSpec(
            num_scalar_prefetch=2,
            grid=(n_batch // n_req,),
            in_specs=[pl.BlockSpec((n_steps, n_req, heads, hd), lambda i, order, rel: (0, order[i], 0, 0)),
                      new_blk, new_blk, cache_in, cache_in],
            out_specs=[cache_blk, cache_blk,
                       pl.BlockSpec((n_req, rows_q, hd), lambda i, order, rel: (i, 0, 0)),
                       pl.BlockSpec((n_req, 1, 2 * rows_q), lambda i, order, rel: (i, 0, 0))],
            scratch_shapes=[pltpu.VMEM((rows_q, rows_c), jnp.int32)] + [pltpu.VMEM((rows_q, rows_c), jnp.float32)] * 2
                           + [pltpu.VMEM((rows_q, rows_c), jnp.bfloat16)] * 2
                           + [cache_buf, cache_buf, pltpu.SemaphoreType.DMA((2, n_buf))],
        ),
        out_shape=[cache_shape, cache_shape,
                   jax.ShapeDtypeStruct((n_batch, rows_q, hd), jnp.float32),
                   jax.ShapeDtypeStruct((n_batch, 1, 2 * rows_q), jnp.float32)],
        compiler_params=pltpu.CompilerParams(dimension_semantics=("arbitrary",), vmem_limit_bytes=62 * 2**20),
        cost_estimate=pl.CostEstimate(flops=4 * n_batch * rows_q * rows_c * hd, bytes_accessed=8 * n_batch * rows_c * hd,
                                      transcendentals=n_batch * rows_q * rows_c),
        name="decode_attention",
    )(order, rel, q, k_new, v_new, k_cache, v_cache)


def tail_kernel(dims, o_hbm, ml_hbm, x_hbm, gain_ref, wo_hbm, wg_hbm, wu_hbm, wd_hbm, out_ref,
                ring, o_ref, ml_ref, x_ref, near1, nml, far1, fml, comb, attn, part_o, recv_o, res, mid, mid_out, mid_in, act,
                part_d, other_d, other_in, fin, across, near, diag,
                ring_sem, om_sem, mm_sem, x_sem, n1s, n1r, nms, nmr, f1s, f1r, fms, fmr, os_, or_, ms_, mr_, ps_, pr_, ds_, dr_, xs_, xr_, cs_, cr_, gs_, gr_):
    n_steps, heads, hd, n_chunks, exp_scale, n_slots = dims
    rows_q = n_steps * heads
    own = far1.shape[0]
    per = own // n_chunks
    tok = per * n_steps
    n_tok, width = res.shape
    hrows = n_tok // 2
    kt, nt = ring.shape[1], ring.shape[2]
    inner = act.shape[1]
    n_o, k_o = width // nt, heads * hd // kt
    n_up, k_up = inner // nt, width // kt
    n_dn, k_dn = width // nt, inner // kt
    first_mlp = n_o * k_o
    up_loads, dn_loads = 2 * k_up * n_up, k_dn * n_dn
    mlp_loads = up_loads + dn_loads
    n_loads = first_mlp + 2 * mlp_loads

    sp = lax.axis_index('sp')
    tp = lax.axis_index('tp')
    core = lax.rem(sp, 2)
    sp_core = sp + 1 - 2 * core
    sp_chip = lax.rem(sp + 2, 4)
    sp_diag = lax.rem(sp_core + 2, 4)
    to_core = {'sp': sp_core}
    to_chip = {'sp': sp_chip}
    to_tp = {'tp': 1 - tp}

    def send(src, dst, s_sem, r_sem, dev):
        return pltpu.make_async_remote_copy(src_ref=src, dst_ref=dst, send_sem=s_sem, recv_sem=r_sem, device_id=dev,
                                            device_id_type=pl.DeviceIdType.MESH)

    barrier = pltpu.get_barrier_semaphore()
    for dev in (to_core, to_chip, to_tp):
        pl.semaphore_signal(barrier, inc=1, device_id=dev, device_id_type=pl.DeviceIdType.MESH)
    pl.semaphore_wait(barrier, 3)

    near_ml = send(ml_hbm.at[pl.ds(0, 2 * own)], nml, nms.at[0], nmr.at[0], to_core)
    near_ml.start()
    near_o = []
    for piece in (0, 1):
        for j in range(n_chunks):
            rows = pl.ds(piece * own + j * per, per)
            near_o.append(send(o_hbm.at[rows], near1.at[rows], n1s.at[piece * n_chunks + j], n1r.at[piece * n_chunks + j], to_core))
    for copy in near_o:
        copy.start()
    mine_ml = pltpu.make_async_copy(ml_hbm.at[pl.ds(2 * own, 2 * own)], ml_ref, mm_sem.at[0])
    mine_ml.start()
    mine_o = [pltpu.make_async_copy(o_hbm.at[pl.ds((2 + piece) * own, own)], o_ref.at[pl.ds(piece * own, own)], om_sem.at[piece])
              for piece in (0, 1)]
    mine_o[0].start()
    mine_o[1].start()

    def load_x(j, step):
        return pltpu.make_async_copy(x_hbm.at[step, pl.ds(pl.multiple_of(sp * own + j * per, per), per)], x_ref.at[j * n_steps + step],
                                     x_sem.at[j * n_steps + step])

    for j in range(n_chunks):
        for step in range(n_steps):
            load_x(j, step).start()

    def load(src, row, col, slot):
        return pltpu.make_async_copy(src.at[pl.ds(pl.multiple_of(row, kt), kt), pl.ds(pl.multiple_of(col, nt), nt)],
                                     ring.at[slot], ring_sem.at[slot])

    def start(idx):
        slot = lax.rem(idx, n_slots)

        @pl.when(idx < first_mlp)
        def _():
            load(wo_hbm, lax.rem(idx, k_o) * kt, (idx // k_o) * nt, slot).start()

        loc = lax.rem(idx - first_mlp + mlp_loads, mlp_loads)
        in_mlp = (idx >= first_mlp) & (idx < n_loads)
        sub = lax.rem(loc, 2 * k_up)
        up_col = core * inner + (loc // (2 * k_up)) * nt

        @pl.when(in_mlp & (loc < up_loads) & (sub < k_up))
        def _():
            load(wg_hbm, sub * kt, up_col, slot).start()

        @pl.when(in_mlp & (loc < up_loads) & (sub >= k_up))
        def _():
            load(wu_hbm, (sub - k_up) * kt, up_col, slot).start()

        dn = loc - up_loads

        @pl.when(in_mlp & (loc >= up_loads))
        def _():
            load(wd_hbm, core * inner + lax.rem(dn, k_dn) * kt, (dn // k_dn) * nt, slot).start()

    def arrived(idx):
        slot = lax.rem(idx, n_slots)
        load(wo_hbm, 0, 0, slot).wait()
        return slot

    def start_many(lo, hi):
        def one(i, carry):
            start(i)
            return carry
        lax.fori_loop(lo, hi, one, 0)

    start_many(0, n_slots)

    diag_mask = lax.broadcasted_iota(jnp.int32, (rows_q, 2 * rows_q), 0) == lax.broadcasted_iota(jnp.int32, (rows_q, 2 * rows_q), 1)
    left = lax.broadcasted_iota(jnp.int32, (per, 2 * rows_q), 1) < rows_q

    def column(row):
        return jnp.sum(jnp.where(diag_mask, row, 0.0), axis=1, keepdims=True)

    def weights(stat_a, stat_b):
        top = jnp.maximum(stat_a, stat_b)
        wt_a = jnp.exp2((stat_a - top) * exp_scale)
        wt_b = jnp.exp2((stat_b - top) * exp_scale)
        total = pltpu.roll(wt_a, rows_q, 1) * stat_a + pltpu.roll(wt_b, rows_q, 1) * stat_b
        return wt_a, wt_b, jnp.where(left, top, total)

    def merge_near(piece, j):
        base = piece * own + j * per
        near_o[piece * n_chunks + j].wait_recv()
        wt_a, wt_b, stat = weights(nml[base:base + per, :], ml_ref[base:base + per, :])
        nml[base:base + per, :] = stat
        for i in range(per):
            near1[base + i] = column(wt_a[i:i + 1]) * near1[base + i] + column(wt_b[i:i + 1]) * o_ref[base + i]

    near_ml.wait_recv()
    mine_ml.wait()
    mine_o[0].wait()
    far_o, far_ml = [], []
    for j in range(n_chunks):
        rows = pl.ds(j * per, per)
        merge_near(0, j)
        far_ml.append(send(nml.at[rows], fml.at[rows], fms.at[j], fmr.at[j], to_chip))
        far_o.append(send(near1.at[rows], far1.at[rows], f1s.at[j], f1r.at[j], to_chip))
        far_ml[j].start()
        far_o[j].start()
    mine_o[1].wait()
    for j in range(n_chunks):
        merge_near(1, j)

    def tp_o(j, n):
        return send(part_o.at[j, n], recv_o.at[j, n], os_.at[j, n], or_.at[j, n], to_tp)

    for j in range(n_chunks):
        base = j * per
        far_ml[j].wait_recv()
        far_o[j].wait_recv()
        wt_a, wt_b, stat = weights(nml[own + base:own + base + per, :], fml[base:base + per, :])
        inv = pltpu.roll(1.0 / stat, rows_q, 1)
        wt_a, wt_b = wt_a * inv, wt_b * inv
        for i in range(per):
            comb[i * rows_q:(i + 1) * rows_q, :] = (column(wt_a[i:i + 1]) * near1[own + base + i]
                                                    + column(wt_b[i:i + 1]) * far1[base + i])
        for step in range(n_steps):
            for h in range(heads):
                attn[step * per:(step + 1) * per, h * hd:(h + 1) * hd] = comb[pl.ds(step * heads + h, per, stride=rows_q), :]
        attn_in = attn[...].astype(jnp.bfloat16)

        def o_tile(n, carry, j=j, attn_in=attn_in):
            acc = None
            for k in range(k_o):
                if j == 0:
                    arrived(n * k_o + k)
                prod = jnp.dot(attn_in[:, k * kt:(k + 1) * kt], ring[n * k_o + k], preferred_element_type=jnp.float32)
                acc = prod if acc is None else acc + prod
            part_o[j, n] = acc
            tp_o(j, n).start()
            return carry
        lax.fori_loop(0, n_o, o_tile, 0)
    start_many(n_slots, n_slots + first_mlp)

    mid_x = [send(mid_out.at[j], mid_in.at[j], ms_.at[j], mr_.at[j], to_core) for j in range(n_chunks)]

    def pair_d(h, t):
        return send(other_d.at[h, t], other_in.at[h, t], ps_.at[h, t], pr_.at[h, t], to_core)

    def tp_d(h, t):
        return send(part_d.at[h, t], fin.at[h, t], ds_.at[h, t], dr_.at[h, t], to_tp)

    def chip_d(h, t):
        return send(fin.at[h, t], across.at[h, t], xs_.at[h, t], xr_.at[h, t], to_chip)

    def core_d(h, t):
        return send(fin.at[h, t], near.at[h, t], cs_.at[h, t], cr_.at[h, t], to_core)

    def diag_d(h, t):
        return send(across.at[h, t], diag.at[h, t], gs_.at[h, t], gr_.at[h, t], to_core)

    def cols(t):
        return pl.ds(t * nt if isinstance(t, int) else pl.multiple_of(t * nt, nt), nt)

    def emit(who, h, t, value):
        for c in (0, 1):
            for step in range(n_steps):
                low = c * tok + step * per
                out_ref[step * 4 * n_chunks + who * n_chunks + 2 * h + c, :, cols(t)] = value[low:low + per].astype(out_ref.dtype)

    def loop(lo, hi, fn):
        def one(t, carry):
            fn(t)
            return carry
        lax.fori_loop(lo, hi, one, 0)

    half = 16

    def residual(j):
        for step in range(n_steps):
            load_x(j, step).wait()
        loop(0, n_o, lambda n: tp_o(j, n).wait_recv())
        h, low = j // 2, (j % 2) * tok

        def norm_rows(i, carry):
            sub = pl.ds(pl.multiple_of(i * half, half), half)
            rows = pl.ds(pl.multiple_of(j * tok + i * half, half), half)
            base = j * n_steps + i * (half // per)
            x_rows = jnp.concatenate([x_ref[base + g].astype(jnp.float32) for g in range(half // per)], axis=0)
            proj = jnp.concatenate([part_o[j, n, sub, :] + recv_o[j, n, sub, :] for n in range(n_o)], axis=1)
            summed = x_rows + proj
            resid = summed.astype(jnp.bfloat16)
            res[rows, :] = resid
            wide = resid.astype(jnp.float32)
            inv = lax.rsqrt(jnp.mean(wide * wide, axis=-1, keepdims=True) + NORM_EPS)
            scaled = wide * inv * gain_ref[...].astype(jnp.float32)
            mid_out[j, sub, :] = scaled
            mid[h, pl.ds(pl.multiple_of(low + i * half, half), half), :] = scaled.astype(jnp.bfloat16)
            return carry
        lax.fori_loop(0, tok // half, norm_rows, 0)
        mid_x[j].start()

    def partner(j):
        mid_x[j].wait_recv()
        h, low = j // 2, hrows + (j % 2) * tok

        def copy_rows(i, carry):
            sub = pl.ds(pl.multiple_of(i * half, half), half)
            mid[h, pl.ds(pl.multiple_of(low + i * half, half), half), :] = mid_in[j, sub, :].astype(jnp.bfloat16)
            return carry
        lax.fori_loop(0, tok // half, copy_rows, 0)

    def up_tile(h, t):
        idx = first_mlp + h * mlp_loads + 2 * k_up * t
        total = []
        for side in (0, 1):
            acc = None
            for k in range(k_up):
                slot = arrived(idx + side * k_up + k)
                prod = jnp.dot(mid[h, :, k * kt:(k + 1) * kt], ring[slot], preferred_element_type=jnp.float32)
                acc = prod if acc is None else acc + prod
            total.append(acc)
        gate, up = total
        act[:, cols(t)] = (jax.nn.silu(gate) * up).astype(jnp.bfloat16)
        for k in range(2 * k_up):
            start(idx + k + n_slots)

    def down(h, t):
        idx = first_mlp + h * mlp_loads + up_loads + k_dn * t
        acc = None
        for k in range(k_dn):
            slot = arrived(idx + k)
            prod = jnp.dot(act[:, k * kt:(k + 1) * kt], ring[slot], preferred_element_type=jnp.float32)
            acc = prod if acc is None else acc + prod
        part_d[h, t] = acc[:hrows]
        other_d[h, t] = acc[hrows:]
        pair_d(h, t).start()
        for k in range(k_dn):
            start(idx + k + n_slots)

    def reduce(h, t):
        pair_d(h, t).wait_recv()
        part_d[h, t] = part_d[h, t] + other_in[h, t]
        tp_d(h, t).start()

    def finish(h, t):
        tp_d(h, t).wait_recv()
        fin[h, t] = res[h * hrows:(h + 1) * hrows, cols(t)].astype(jnp.float32) + (part_d[h, t] + fin[h, t])
        chip_d(h, t).start()
        core_d(h, t).start()
        emit(sp, h, t, fin[h, t])

    def forward(h, t):
        chip_d(h, t).wait_recv()
        diag_d(h, t).start()
        emit(sp_chip, h, t, across[h, t])
        core_d(h, t).wait_recv()
        emit(sp_core, h, t, near[h, t])

    def collect(h, t):
        diag_d(h, t).wait_recv()
        emit(sp_diag, h, t, diag[h, t])

    def down_then_reduce(h):
        def one(t):
            down(h, t)
            reduce(h, t - 1)
        return one

    for j in (0, 1):
        residual(j)
    for j in (0, 1):
        partner(j)
    loop(0, n_up, lambda t: up_tile(0, t))
    down(0, 0)
    loop(1, n_dn, down_then_reduce(0))
    reduce(0, n_dn - 1)

    for j in (2, 3):
        residual(j)
    for j in (2, 3):
        partner(j)
    up_tile(1, 0)

    def up_then_finish(t):
        up_tile(1, t)
        finish(0, t - 1)

    loop(1, n_up, up_then_finish)
    down(1, 0)
    finish(0, n_up - 1)

    def down_more(t):
        down(1, t)
        reduce(1, t - 1)

    loop(1, 3, down_more)
    finish(0, n_up)
    loop(3, 5, down_more)
    finish(0, n_up + 1)
    loop(5, n_dn, down_more)
    reduce(1, n_dn - 1)
    loop(0, n_dn // 2, lambda t: forward(0, t))

    def wind_a(t):
        finish(1, t)
        forward(0, t + n_dn // 2)

    loop(0, n_dn // 2, wind_a)

    def wind_b(t):
        finish(1, t)
        forward(1, t - n_dn // 2)
        collect(0, t - n_dn // 2)

    loop(n_dn // 2, n_dn, wind_b)

    def wind_c(t):
        collect(0, t)
        forward(1, t)
        collect(1, t - n_dn // 2)

    loop(n_dn // 2, n_dn, wind_c)
    loop(n_dn // 2, n_dn, lambda t: collect(1, t))

    for copy in near_o + [near_ml] + far_o + far_ml + mid_x:
        copy.wait_send()
    for j in range(n_chunks):
        loop(0, n_o, lambda n, j=j: tp_o(j, n).wait_send())
    for h in (0, 1):
        for build in (pair_d, tp_d, chip_d, core_d, diag_d):
            loop(0, n_dn, lambda t, h=h, build=build: build(h, t).wait_send())


def finish_layer(o_part, ml, hidden, norm, w_o, w_gate, w_up, w_down, heads, exp_scale):
    n_batch, rows_q, hd = o_part.shape
    n_steps, _, width = hidden.shape
    own = n_batch // 4
    tokens = own * n_steps
    inner = w_gate.shape[1] // 2
    n_chunks, n_slots, kt, nt = 4, 20, 1024, 512
    per = own // n_chunks
    n_dn = width // nt
    vmem = pl.BlockSpec(memory_space=pltpu.VMEM)
    hbm = pl.BlockSpec(memory_space=pl.ANY)
    f32, bf16 = jnp.float32, jnp.bfloat16
    tiles = pltpu.VMEM((2, n_dn, tokens // 2, nt), f32)
    chunk = pltpu.VMEM((n_chunks, per * n_steps, width), f32)
    o_tiles = pltpu.VMEM((n_chunks, n_dn, per * n_steps, nt), f32)
    dma = pltpu.SemaphoreType.DMA
    return pl.pallas_call(
        functools.partial(tail_kernel, (n_steps, heads, hd, n_chunks, exp_scale, n_slots)),
        in_specs=[hbm] * 3 + [vmem] + [hbm] * 4,
        out_specs=vmem,
        out_shape=jax.ShapeDtypeStruct((n_steps * n_batch // per, per, width), bf16),
        scratch_shapes=[pltpu.VMEM((n_slots, kt, nt), bf16),
                        pltpu.VMEM((2 * own, rows_q, hd), f32), pltpu.VMEM((2 * own, 2 * rows_q), f32),
                        pltpu.VMEM((n_chunks * n_steps, per, width), bf16),
                        pltpu.VMEM((2 * own, rows_q, hd), f32), pltpu.VMEM((2 * own, 2 * rows_q), f32),
                        pltpu.VMEM((own, rows_q, hd), f32), pltpu.VMEM((own, 2 * rows_q), f32),
                        pltpu.VMEM((per * rows_q, hd), f32),
                        pltpu.VMEM((per * n_steps, heads * hd), f32),
                        o_tiles, o_tiles,
                        pltpu.VMEM((tokens, width), bf16), pltpu.VMEM((2, tokens, width), bf16), chunk, chunk,
                        pltpu.VMEM((tokens, inner), bf16),
                        tiles, tiles, tiles, tiles, tiles, tiles, tiles,
                        dma((n_slots,)), dma((2,)), dma((1,)), dma((n_chunks * n_steps,)),
                        dma((2 * n_chunks,)), dma((2 * n_chunks,)), dma((1,)), dma((1,)),
                        dma((n_chunks,)), dma((n_chunks,)), dma((n_chunks,)), dma((n_chunks,)), dma((n_chunks, n_dn)), dma((n_chunks, n_dn)),
                        dma((n_chunks,)), dma((n_chunks,))] + [dma((2, n_dn))] * 10,
        compiler_params=pltpu.CompilerParams(collective_id=0, has_side_effects=True, vmem_limit_bytes=63 * 2**20),
        name="finish_layer",
    )(o_part, ml, hidden, norm, w_o, w_gate, w_up, w_down)


def solution(mesh):
    cache_spec = P('dp', 'sp', 'tp', None)
    col_spec = P(None, 'tp')
    row_spec = P('tp', None)
    in_specs = (P(None, 'dp', None), P('dp'), cache_spec, cache_spec, col_spec, col_spec, col_spec, row_spec,
                col_spec, col_spec, row_spec, P(), P(), P(), P())
    out_specs = (P(None, 'dp', None), cache_spec, cache_spec)

    def shard_body(hidden, start_pos, k_cache, v_cache, w_q, w_k, w_v, w_o, w_gate, w_up, w_down, attn_norm, mlp_norm, q_gain, k_gain):
        n_steps, n_batch, width = hidden.shape
        seq_blk, kv_heads, hd = k_cache.shape[1], k_cache.shape[2], k_cache.shape[3]
        heads = w_q.shape[1] // hd
        rows_q = n_steps * heads
        exp_scale = hd ** -0.5 * math.log2(math.e)
        sp = lax.axis_index('sp')
        core, chip = sp % 2, sp // 2
        own = n_batch // 4

        tok_pos = (start_pos[None, :] + jnp.arange(n_steps, dtype=jnp.int32)[:, None]).reshape(-1)
        cos_tab, sin_tab = rope_tables(tok_pos, hd)
        q_rows, k_rows, v_rows = project_qkv(hidden.reshape(n_steps * n_batch, width), attn_norm.reshape(1, width), cos_tab, sin_tab,
                                             q_gain, k_gain, w_q, w_k, w_v)
        q_rot = q_rows.reshape(n_steps, n_batch, heads, hd)
        k_rows = k_rows.reshape(n_steps, n_batch * kv_heads, hd)
        v_rows = v_rows.reshape(n_steps, n_batch * kv_heads, hd)

        n_req = 4
        per = own // n_req
        part = jnp.stack([(1 - chip) * 2 + (1 - core), chip * 2 + (1 - core), (1 - chip) * 2 + core, chip * 2 + core])
        order = (part[:, None] * per + jnp.arange(per)[None, :]).reshape(-1).astype(jnp.int32)
        rel = start_pos - sp * seq_blk
        flat = (n_batch, seq_blk * kv_heads, hd)
        k_out, v_out, o_part, ml = attention(order, rel, q_rot, k_rows, v_rows, k_cache.reshape(flat), v_cache.reshape(flat),
                                             kv_heads, exp_scale, n_req)

        hid_out = finish_layer(o_part, ml.reshape(n_batch, 2 * rows_q), hidden, mlp_norm.reshape(1, width), w_o, w_gate, w_up, w_down,
                               heads, exp_scale).reshape(hidden.shape)
        return hid_out, k_out.reshape(k_cache.shape), v_out.reshape(v_cache.shape)

    return jax.shard_map(shard_body, mesh=mesh, in_specs=in_specs, out_specs=out_specs, check_vma=False)
```
